32 devices in a mesh: col: 8 (over y, x, core), grp: 4 (over z).
Axes of the slice: x: 2, y: 2, z: 4, core: 2. Of those that a mesh axis runs over, the one named last changes fastest.
Arguments:
- profiles: float32 [2048, 116], P('col'), may hold values from -6 to 6
- courant: float32 [2048, 58], P('col'), may hold values from -0.7 to 0.7
- owner_map: int32 [2048], replicated, may hold values from 0 to 2047, as said below
- cloud_flags: int32 [2048], P('col'), may hold values 0 or 1
- crm_state: float32 [2, 58, 64, 2048], P(None, None, 'grp', 'col'), may hold values from -6 to 6
Outputs:
- tendency: float32 [2048, 116], P('col')
- crm_final: float32 [2, 58, 64, 2048], P(None, None, 'grp', 'col')
The draws below stay inside these ranges and needn't reach their ends.
Inputs may be any that keep to these rules, and one draw needn't show every extreme that they name: owner_map is a permutation; physics column p lives in span p // 256, element column e in group e // 256; each group hands at most 34 columns to one span, and exactly 34 to some spans, and every span receives exactly 256 columns.
All inputs are finite; a program needn't handle non-finite values. No bound on the sum of `cloud_flags` on one device may be relied on, other than what follows from the above.
Results may differ from the reference program's by a relative error of at most 0.00002.
Values sent between devices are 32-bit elements; how exact they have to be, the bound alone decides.
A program may use at most 64 MiB of HBM per device.

```python
import jax
import jax.numpy as jnp

NX = 64
NZ = 58
COLS_DEV = 256
STEPS = 8
COLUMNS = 2048


def draw_owner_map(key, part):
    per_block = COLS_DEV
    block_count = COLUMNS // COLS_DEV
    mean_load = per_block // block_count
    excess = min(2, mean_load)
    key_pattern, key_offset, key_dest, key_source = jax.random.split(jax.random.fold_in(key, 17), 4)
    block_ids = jnp.arange(block_count, dtype=jnp.int32)
    pattern = jnp.where(block_ids % 2 == 0, mean_load + excess, mean_load - excess).astype(jnp.int32)
    pattern = pattern[jax.random.permutation(key_pattern, block_count)]
    offset_of = jax.random.permutation(key_offset, block_count).astype(jnp.int32)
    counts = pattern[(block_ids[None, :] - offset_of[:, None]) % block_count]
    block_ends = jnp.cumsum(counts, axis=1)
    block_starts = block_ends - counts
    slot_ids = jnp.arange(per_block, dtype=jnp.int32)
    dest_block = jnp.sum((slot_ids[None, :, None] >= block_ends[:, None, :]).astype(jnp.int32), axis=2)
    within = slot_ids[None, :] - jnp.take_along_axis(block_starts, dest_block, axis=1)
    arrival = jnp.cumsum(counts, axis=0) - counts
    slot_in_dest = jnp.take_along_axis(arrival, dest_block, axis=1) + within
    dest_shuffle = jax.vmap(lambda subkey: jax.random.permutation(subkey, per_block))(jax.random.split(key_dest, block_count)).astype(jnp.int32)
    physical = dest_block * per_block + dest_shuffle[dest_block, slot_in_dest]
    source_shuffle = jax.vmap(lambda subkey: jax.random.permutation(subkey, per_block))(jax.random.split(key_source, block_count)).astype(jnp.int32)
    element = block_ids[:, None] * per_block + source_shuffle
    return jnp.zeros((COLUMNS,), jnp.int32).at[element.reshape(-1)].set(physical.reshape(-1).astype(jnp.int32))


def with_ends(values, stream_key, least, largest):
    longest = values.shape.index(max(values.shape))
    spots = []
    for shift in (0, 1):
        where = [jax.random.randint(jax.random.fold_in(stream_key, axis), (), 0, length) for axis, length in enumerate(values.shape)]
        where[longest] = (where[longest] + shift) % values.shape[longest]
        spots.append(tuple(where))
    return values.at[spots[0]].set(least).at[spots[1]].set(largest)


def levels(own_key, extent, pieces, low, high):
    factor_of, own = 1.0, jax.random.fold_in(own_key, 6)
    for axis_at, blocks in pieces:
        draws = jnp.exp(jax.random.uniform(jax.random.fold_in(own, axis_at), (blocks,), jnp.float32, low / len(pieces), high / len(pieces)))
        factor_of = factor_of * jnp.repeat(draws, extent[axis_at] // blocks).reshape([-1 if axis == axis_at else 1 for axis in range(len(extent))])
    return factor_of


def scatter_about(key, extent, width, limit, pieces=(), kind=jnp.bfloat16):
    drawn = width * jax.random.normal(key, extent, jnp.float32)
    if pieces:
        drawn = drawn * levels(key, extent, pieces, -0.22, 0.18)
    return jnp.clip(drawn, -limit, limit).astype(kind)


def setup_inputs(seed: int = 0) -> dict:
    key_of = jax.random.split(jax.random.key(seed), 6)
    return {
        "profiles": scatter_about(key_of[0], (COLUMNS, 2 * NZ), 1.0, 6.0, ((0, 8),), jnp.float32),
        "courant": jnp.clip(jax.random.uniform(key_of[1], (COLUMNS, NZ), jnp.float32, -0.7, 0.7) * levels(key_of[1], (COLUMNS, NZ), ((0, 8),), -0.4, 0.0), -0.7, 0.7),
        "owner_map": draw_owner_map(jax.random.fold_in(key_of[5], 71), 0),
        "cloud_flags": with_ends((jax.random.randint(key_of[3], (COLUMNS,), 0, 2) < 1).astype(jnp.int32), jax.random.fold_in(key_of[3], 1), 0, 1),
        "crm_state": scatter_about(key_of[4], (2, NZ, NX, COLUMNS), 1.0, 6.0, ((2, 4), (3, 8)), jnp.float32),
    }


diffuse_x = 0.25
diffuse_z = 0.2
sat_scale = 0.5
sat_slope = 0.3
cond_rate = 0.5
latent_gain = 0.4


def condense(fields, cloudy):
    energy = fields[0]
    moisture = fields[1]
    saturation = sat_scale * (jnp.exp(sat_slope * energy) - 1.0)
    amount = cond_rate * jnp.maximum(moisture - saturation, 0.0) * cloudy
    return jnp.stack([energy + latent_gain * amount, moisture - amount])


def advance(centre, eastern, western, courant_here, forcing, cloudy):
    upper = jnp.concatenate([centre[:, 1:], centre[:, -1:]], axis=1)
    lower = jnp.concatenate([centre[:, :1], centre[:, :-1]], axis=1)
    stepped = centre + courant_here * ((western - eastern) * 0.5) + diffuse_x * (eastern - 2.0 * centre + western) + diffuse_z * (upper - 2.0 * centre + lower) + forcing
    return condense(stepped, cloudy)


def reference(profiles, courant, owner_map, cloud_flags, crm_state):
    columns = profiles.shape[0]
    phys_prof = jnp.zeros_like(profiles).at[owner_map].set(profiles)
    phys_cour = jnp.zeros_like(courant).at[owner_map].set(courant)
    forcing = (phys_prof.reshape(columns, 2, NZ).transpose(1, 2, 0) / STEPS)[:, :, None, :]
    courant_here = phys_cour.T[None, :, None, :]
    cloudy = cloud_flags.astype(jnp.float32)
    crm_now = crm_state
    for repeat in range(STEPS):
        crm_now = advance(crm_now, jnp.roll(crm_now, -1, axis=2), jnp.roll(crm_now, 1, axis=2), courant_here, forcing, cloudy)
    increment = (jnp.sum(crm_now, axis=2) - jnp.sum(crm_state, axis=2)) / NX
    phys_inc = increment.transpose(2, 0, 1).reshape(columns, 2 * NZ)
    tendency = phys_inc[owner_map]
    return tendency, crm_now
```

```python
import functools

import jax
import jax.numpy as jnp
from jax import lax
from jax.experimental import pallas as pl
from jax.experimental.pallas import tpu as pltpu
from jax.sharding import PartitionSpec as P

STEPS = 8
DEPTH = STEPS
BLOCK = 8
LANES = 128
LIMIT = int(50 * 2**20)
TOP = 8
MESH = pl.DeviceIdType.MESH
HIGHEST = lax.Precision.HIGHEST

diffuse_x = 0.25
diffuse_z = 0.2
sat_scale = 0.5
sat_slope = 0.3
cond_rate = 0.5
latent_gain = 0.4
LOG2E = 1.4426950408889634


def round_up(n, m):
    return -(-n // m) * m


def contract(a, b, dims):
    return lax.dot_general(
        a, b, (dims, ((), ())), precision=HIGHEST, preferred_element_type=jnp.float32
    )


def window_kernel(
    prof_hbm,
    cour_hbm,
    owner_hbm,
    cloud_hbm,
    x_hbm,
    land,
    give,
    final_ref,
    prof_ref,
    cour_ref,
    owner_ref,
    cloud_ref,
    wide,
    slabs,
    odd,
    even,
    take,
    fsend,
    fland,
    force,
    wind,
    part,
    heap,
    mine,
    inc,
    pack,
    local_sem,
    halo_sem,
    force_sem,
    sum_sem,
    back_sem,
):
    fields, levels, cells, columns = x_hbm.shape
    chunks = columns // LANES
    groups, cap = fland.shape[:2]
    peers = lax.axis_size("grp")
    z_me = lax.axis_index("grp")
    c_me = lax.axis_index("col")
    direct = cells % 8 == 0
    reach = 1 if direct else DEPTH // cells
    width = cells + 2 * DEPTH
    own = TOP + DEPTH
    blocks = -(-levels // BLOCK)
    middle = blocks - 2
    tail = levels - (blocks - 1) * BLOCK
    span = lambda i: pl.ds(i * LANES, LANES)

    loads = []
    for c in range(chunks):
        if direct:
            target = wide.at[c, :, :, own : own + cells, :]
        else:
            target = slabs.at[c, 2 * reach]
        load = pltpu.make_async_copy(x_hbm.at[:, :, :, span(c)], target, local_sem.at[c])
        load.start()
        loads.append(load)
    small = []
    pairs = ((prof_hbm, prof_ref), (cour_hbm, cour_ref), (owner_hbm, owner_ref), (cloud_hbm, cloud_ref))
    for i, (source, target) in enumerate(pairs):
        load = pltpu.make_async_copy(source, target, local_sem.at[chunks + i])
        load.start()
        small.append(load)

    barrier = pltpu.get_barrier_semaphore()
    for k in range(1, peers):
        pl.semaphore_signal(
            barrier, inc=1, device_id={"grp": lax.rem(z_me + k, peers)}, device_id_type=MESH
        )
    for k in range(1, groups):
        pl.semaphore_signal(
            barrier, inc=1, device_id={"col": lax.rem(c_me + k, groups)}, device_id_type=MESH
        )

    def halo_copies(c, b, count):
        rows = pl.ds(b * BLOCK, count)
        copies = []
        for j in range(1, reach + 1):
            for side in range(2):
                peer = lax.rem(z_me + (peers - j if side == 0 else j), peers)
                slot = 2 * (j - 1) + side
                if direct:
                    near = own if side == 0 else own + cells - DEPTH
                    far = own + cells if side == 0 else TOP
                    source = wide.at[c, :, rows, near : near + DEPTH, :]
                    target = wide.at[c, :, rows, far : far + DEPTH, :]
                else:
                    source = slabs.at[c, 2 * reach, :, rows]
                    target = slabs.at[c, slot, :, rows]
                copies.append(
                    pltpu.make_async_remote_copy(
                        src_ref=source,
                        dst_ref=target,
                        send_sem=halo_sem.at[0, c, b, slot],
                        recv_sem=halo_sem.at[1, c, b, slot],
                        device_id={"grp": peer},
                        device_id_type=MESH,
                    )
                )
        return copies

    size = lambda b: BLOCK if b < blocks - 1 else tail
    waits = []
    with jax.named_scope("barrier"):
        pl.semaphore_wait(barrier, peers - 1 + groups - 1)
    with jax.named_scope("send"):
        for c in range(chunks):
            loads[c].wait()
            for b in range(blocks):
                for copy in halo_copies(c, b, size(b)):
                    copy.start()
                    waits.append(copy)

    with jax.named_scope("forcing"):
        for load in small:
            load.wait()
        owner = jnp.concatenate(
            [owner_ref[pl.ds(c, groups, stride=chunks), :] for c in range(chunks)], axis=1
        )
        own_row = jnp.concatenate(
            [owner_ref[pl.ds(c_me * chunks + c, 1), :] for c in range(chunks)], axis=1
        )
        group_ids = lax.broadcasted_iota(jnp.int32, (groups, columns), 0)
        earlier = (
            lax.broadcasted_iota(jnp.int32, (columns, columns), 0)
            < lax.broadcasted_iota(jnp.int32, (columns, columns), 1)
        ).astype(jnp.float32)
        slot = lax.broadcasted_iota(jnp.int32, (cap, columns), 0).astype(jnp.float32)
        spot = lax.broadcasted_iota(jnp.int32, (cap, columns), 1).astype(jnp.float32) + 1.0

        def ranked(hits):
            rank = jnp.dot(hits, earlier, preferred_element_type=jnp.float32)
            return jnp.where(hits > 0.5, rank, -1.0)

        low = own_row - group_ids * columns
        order = ranked(jnp.where((low >= 0) & (low < columns), 1.0, 0.0))
        for q in range(groups):
            give[q * cap : (q + 1) * cap, :] = jnp.where(order[q : q + 1] == slot, 1.0, 0.0)

        for f, ref in ((0, prof_ref), (1, cour_ref)):
            lines = ref.shape[0]
            fsend[:, :, f * LANES : f * LANES + lines] = contract(
                give[...], ref[...], ((1,), (1,))
            ).reshape(groups, cap, lines)
        shares = []
        for k in range(1, groups):
            peer = lax.rem(c_me + k, groups)
            copy = pltpu.make_async_remote_copy(
                src_ref=fsend.at[peer],
                dst_ref=fland.at[c_me],
                send_sem=force_sem.at[0, k],
                recv_sem=force_sem.at[1, k],
                device_id={"col": peer},
                device_id_type=MESH,
            )
            copy.start()
            shares.append(copy)
        waits += shares
        fland[c_me] = fsend[c_me]

        local = owner - c_me * columns
        order = ranked(jnp.where((local >= 0) & (local < columns), 1.0, 0.0))
        place = (local + 1).astype(jnp.float32)
        for q in range(groups):
            chosen = jnp.where(order[q : q + 1] == slot, place[q : q + 1], 0.0)
            chosen = jnp.sum(chosen, axis=1, keepdims=True)
            take[q * cap : (q + 1) * cap, :] = jnp.where(chosen == spot, 1.0, 0.0)

    with jax.named_scope("force_wait"):
        for copy in shares:
            copy.wait_recv()
    with jax.named_scope("force_take"):
        phys = contract(
            fland[:, :, :LANES].reshape(groups * cap, LANES), take[...], ((0,), (0,))
        )
        for f in range(fields):
            for c in range(chunks):
                force[c, f] = (
                    phys[f * levels : (f + 1) * levels, c * LANES : (c + 1) * LANES] / STEPS
                )
        phys = contract(
            fland[:, :, LANES:].reshape(groups * cap, LANES), take[...], ((0,), (0,))
        )
        for c in range(chunks):
            wind[c] = phys[:levels, c * LANES : (c + 1) * LANES]
    half_cloud = cond_rate * cloud_ref[...].astype(jnp.float32)

    def stepped(c, s, z):
        rows = width - 2 * s if s == STEPS else round_up(width - 2 * s, 8)
        first = TOP + (width - rows) // 2
        source = wide.at[c] if s == 1 else (odd if s % 2 == 0 else even)
        up = jnp.minimum(z + 1, levels - 1)
        down = jnp.maximum(z - 1, 0)
        speed = 0.5 * wind[c, pl.ds(z, 1), :]
        new = []
        for f in range(fields):
            here = source[f, z, first : first + rows]
            west = source[f, z, first - 1 : first - 1 + rows]
            east = source[f, z, first + 1 : first + 1 + rows]
            upper = source[f, up, first : first + rows]
            lower = source[f, down, first : first + rows]
            new.append(
                (1.0 - 2.0 * diffuse_x - 2.0 * diffuse_z) * here
                + ((diffuse_x + speed) * west + (diffuse_x - speed) * east)
                + (diffuse_z * (upper + lower) + force[c, f, pl.ds(z, 1), :])
            )
        energy, moisture = new
        excess = (moisture + sat_scale) - sat_scale * jnp.exp2((sat_slope * LOG2E) * energy)
        amount = jnp.maximum(excess, 0.0) * half_cloud[:, c * LANES : (c + 1) * LANES]
        return first, rows, (energy + latent_gain * amount, moisture - amount)

    def put(c, s, z, result):
        first, rows, values = result
        target = odd if s % 2 else even
        for f, value in enumerate(values):
            if s == STEPS:
                final_ref[f, z, :, c * LANES : (c + 1) * LANES] = value
                if direct:
                    old = wide[c, f, z, own : own + cells]
                else:
                    old = slabs[c, 2 * reach, f, z]
                part[c, pl.ds(f * levels + z, 1), :] = jnp.sum(
                    value - old, axis=0, keepdims=True
                )
            else:
                target[f, z, first : first + rows] = value

    def sweep(c, s, low, count):
        def pair(i, carry):
            z = low + 2 * i
            results = [stepped(c, s, z + k) for k in range(2)]
            for k in range(2):
                put(c, s, z + k, results[k])
            return carry

        if count > 1:
            lax.fori_loop(0, count // 2, pair, 0)
        if count % 2:
            z = low + count - 1
            put(c, s, z, stepped(c, s, z))

    def arrive(c, b, count):
        for copy in halo_copies(c, b, count):
            copy.wait_recv()
        if not direct:

            def fill(z, carry):
                for f in range(fields):
                    wide[c, f, z, own : own + cells] = slabs[c, 2 * reach, f, z]
                    for j in range(1, reach + 1):
                        right = own + j * cells
                        left = own - j * cells
                        wide[c, f, z, right : right + cells] = slabs[c, 2 * j - 2, f, z]
                        wide[c, f, z, left : left + cells] = slabs[c, 2 * j - 1, f, z]
                return carry

            lax.fori_loop(b * BLOCK, b * BLOCK + count, fill, 0)

    def wave(c):
        with jax.named_scope(f"first#c={c}"):
            arrive(c, 0, BLOCK)
            for s in range(1, STEPS + 1):
                sweep(c, s, 0, BLOCK - s)

        def body(b, carry):
            with jax.named_scope("arrive"):
                arrive(c, b, BLOCK)
            with jax.named_scope("steps"):
                for s in range(1, STEPS + 1):
                    sweep(c, s, b * BLOCK - s, BLOCK)
            return carry

        lax.fori_loop(1, blocks - 1, body, 0)
        with jax.named_scope("arrive_last"):
            arrive(c, blocks - 1, tail)
        with jax.named_scope("steps_last"):
            for s in range(1, STEPS + 1):
                sweep(c, s, (blocks - 1) * BLOCK - s, tail + s)

    lines = part.shape[1] // peers
    block = lambda i: pl.ds(pl.multiple_of(i * lines, lines), lines)

    def sum_copies(c, phase):
        copies = []
        for k in range(1, peers):
            peer = lax.rem(z_me + k, peers)
            if phase == 0:
                source, target = part.at[c, block(peer)], heap.at[c, k]
            else:
                source, target = mine.at[c], inc.at[c, block(z_me)]
            copies.append(
                pltpu.make_async_remote_copy(
                    src_ref=source,
                    dst_ref=target,
                    send_sem=sum_sem.at[phase, 0, c, k],
                    recv_sem=sum_sem.at[phase, 1, c, k],
                    device_id={"grp": peer},
                    device_id_type=MESH,
                )
            )
        for copy in copies:
            copy.start()
            waits.append(copy)
        return copies

    def add_up(c, scatter):
        total = part[c, block(z_me), :]
        for k, copy in enumerate(scatter):
            copy.wait_recv()
            total = total + heap[c, k + 1]
        total = total / (cells * peers)
        mine[c] = total
        inc[c, block(z_me), :] = total
        return sum_copies(c, 1)

    pad_rows = part.shape[1] - fields * levels
    if pad_rows:
        for c in range(chunks):
            part[c, fields * levels :, :] = jnp.zeros((pad_rows, LANES), jnp.float32)

    scatters, gathers = [], []
    for c in range(chunks):
        wave(c)
        scatters.append(sum_copies(c, 0))
    with jax.named_scope("add_up"):
        for c in range(chunks):
            gathers += add_up(c, scatters[c])
    with jax.named_scope("gather_wait"):
        for copy in gathers:
            copy.wait_recv()
    with jax.named_scope("pack"):
        packed = 0.0
        for c in range(chunks):
            packed = packed + contract(
                take[:, c * LANES : (c + 1) * LANES], inc[c], ((1,), (1,))
            )
        pack[...] = packed.reshape(pack.shape)
    returns = []
    for k in range(1, groups):
        peer = lax.rem(c_me + k, groups)
        copy = pltpu.make_async_remote_copy(
            src_ref=pack.at[peer],
            dst_ref=land.at[c_me],
            send_sem=back_sem.at[0, k],
            recv_sem=back_sem.at[1, k],
            device_id={"col": peer},
            device_id_type=MESH,
        )
        copy.start()
        returns.append(copy)
    waits += returns
    land[c_me] = pack[c_me]
    with jax.named_scope("return_wait"):
        for copy in returns:
            copy.wait_recv()
    with jax.named_scope("drain"):
        for copy in waits:
            copy.wait_send()


def finish_kernel(land_ref, give_ref, state_ref, tend_ref, final_ref, sems):
    fields = state_ref.shape[0]
    store = [
        pltpu.make_async_copy(state_ref.at[f], final_ref.at[f], sems.at[f]) for f in range(fields)
    ]
    for copy in store:
        copy.start()
    groups, cap, rows = land_ref.shape
    back = contract(land_ref[...].reshape(groups * cap, rows), give_ref[...], ((0,), (0,)))
    tend_ref[...] = back[: tend_ref.shape[0]]
    for copy in store:
        copy.wait()


def on_device(profiles, courant, owner_map, cloud_flags, crm_state):
    columns = profiles.shape[0]
    fields, levels, cells = crm_state.shape[:3]
    groups = lax.axis_size("col")
    peers = lax.axis_size("grp")
    per_peer = columns // groups
    cap = round_up(per_peer + min(2, per_peer), 8)
    chunks = columns // LANES
    direct = cells % 8 == 0
    reach = 1 if direct else DEPTH // cells
    blocks = -(-levels // BLOCK)
    rows = round_up(fields * levels, 8 * peers)
    f32 = lambda *shape: pltpu.VMEM(shape, jnp.float32)
    i32 = lambda *shape: pltpu.VMEM(shape, jnp.int32)
    dma = lambda *shape: pltpu.SemaphoreType.DMA(shape)
    vmem = pl.BlockSpec(memory_space=pltpu.VMEM)
    anywhere = pl.BlockSpec(memory_space=pl.ANY)
    tall = round_up(TOP + cells + 2 * DEPTH + 1, 8)
    slabs = (8, 128) if direct else (chunks, 2 * reach + 1, fields, levels, cells, LANES)
    land, give, state = pl.pallas_call(
        window_kernel,
        out_shape=(
            jax.ShapeDtypeStruct((groups, cap, rows), jnp.float32),
            jax.ShapeDtypeStruct((groups * cap, columns), jnp.float32),
            jax.ShapeDtypeStruct(crm_state.shape, jnp.float32),
        ),
        in_specs=[anywhere] * 5,
        out_specs=(vmem, vmem, vmem),
        scratch_shapes=[
            f32(fields * levels, columns),
            f32(levels, columns),
            i32(groups * chunks, LANES),
            i32(1, columns),
            f32(chunks, fields, levels, tall, LANES),
            f32(*slabs),
            f32(fields, levels, tall, LANES),
            f32(fields, levels, tall, LANES),
            f32(groups * cap, columns),
            f32(groups, cap, 2 * LANES),
            f32(groups, cap, 2 * LANES),
            f32(chunks, fields, levels, LANES),
            f32(chunks, levels, LANES),
            f32(chunks, rows, LANES),
            f32(chunks, peers, rows // peers, LANES),
            f32(chunks, rows // peers, LANES),
            f32(chunks, rows, LANES),
            f32(groups, cap, rows),
            dma(chunks + 4),
            dma(2, chunks, blocks, 2 * reach),
            dma(2, groups),
            dma(2, 2, chunks, peers),
            dma(2, groups),
        ],
        compiler_params=pltpu.CompilerParams(
            collective_id=0, has_side_effects=True, vmem_limit_bytes=LIMIT
        ),
    )(
        profiles.T,
        courant.T,
        owner_map.reshape(groups * chunks, LANES),
        cloud_flags[None, :],
        crm_state,
    )
    tendency, final = pl.pallas_call(
        finish_kernel,
        out_shape=(
            jax.ShapeDtypeStruct((fields * levels, columns), jnp.float32),
            jax.ShapeDtypeStruct(crm_state.shape, jnp.float32),
        ),
        in_specs=[vmem, vmem, anywhere],
        out_specs=(vmem, anywhere),
        scratch_shapes=[dma(fields)],
        compiler_params=pltpu.CompilerParams(vmem_limit_bytes=4 * 2**20),
    )(land, give, state)
    return tendency.T, final


def solution(mesh):
    placed = (P("col", None), P("col", None), P(), P("col"), P(None, None, "grp", "col"))
    return jax.shard_map(
        on_device,
        mesh=mesh,
        in_specs=placed,
        out_specs=(P("col", None), P(None, None, "grp", "col")),
        check_vma=False,
    )
```

```python
import jax
import jax.numpy as jnp
from jax import lax
from jax.experimental import pallas as pl
from jax.experimental.pallas import tpu as pltpu
from jax.sharding import PartitionSpec as P

STEPS = 8
DEPTH = STEPS
BLOCK = 8
PIECE = 4
LANES = 128
LIMIT = 67_043_328
TOP = 8
MESH = pl.DeviceIdType.MESH

diffuse_x = 0.25
diffuse_z = 0.2
sat_scale = 0.5
sat_slope = 0.3
cond_rate = 0.5
latent_gain = 0.4
SCALE = sat_slope * 1.4426950408889634


def round_up(n, m):
    return -(-n // m) * m


def parts_of(x):
    high = x.astype(jnp.bfloat16)
    rest = x - high.astype(jnp.float32)
    middle = rest.astype(jnp.bfloat16)
    return high, middle, (rest - middle.astype(jnp.float32)).astype(jnp.bfloat16)


def pick(parts, hot, dims, swap=False):
    total = 0.0
    for part in parts:
        pair = (hot, part) if swap else (part, hot)
        total = total + lax.dot_general(
            *pair, (dims, ((), ())), preferred_element_type=jnp.float32
        )
    return total


def level_edges(levels):
    full = max(2, (levels - BLOCK) // BLOCK)
    edges = [i * BLOCK for i in range(full + 1)]
    while edges[-1] < levels:
        edges.append(min(edges[-1] + PIECE, levels))
    return full, edges


def window_kernel(
    prof_hbm,
    cour_hbm,
    owner_hbm,
    cloud_hbm,
    x_hbm,
    land,
    give_hbm,
    final_hbm,
    prof_ref,
    cour_ref,
    owner_ref,
    cloud_ref,
    wide,
    slabs,
    odd,
    even,
    outs,
    give,
    take,
    fsend,
    fland,
    coef,
    whole,
    early,
    late,
    heap,
    early_heap,
    late_heap,
    mine,
    early_mine,
    inc,
    early_inc,
    pack,
    load_sem,
    out_sem,
    halo_send,
    halo_recv,
    swap_sem,
    sum_sem,
):
    fields, levels, cells, columns = x_hbm.shape
    chunks = columns // LANES
    groups, cap = fland.shape[:2]
    peers = lax.axis_size("grp")
    z_me = lax.axis_index("grp")
    c_me = lax.axis_index("col")
    direct = cells % 8 == 0
    reach = 1 if direct else DEPTH // cells
    width = cells + 2 * DEPTH
    own = TOP + DEPTH
    full, edges = level_edges(levels)
    split = (full - 1) * BLOCK
    span = lambda i: pl.ds(i * LANES, LANES)

    loads = []
    for c in range(chunks):
        if direct:
            target = wide.at[c, :, :, own : own + cells, :]
        else:
            target = slabs.at[c, 2 * reach]
        load = pltpu.make_async_copy(x_hbm.at[:, :, :, span(c)], target, load_sem.at[c])
        load.start()
        loads.append(load)
    small = []
    pairs = ((prof_hbm, prof_ref), (cour_hbm, cour_ref), (owner_hbm, owner_ref), (cloud_hbm, cloud_ref))
    for i, (source, target) in enumerate(pairs):
        load = pltpu.make_async_copy(source, target, load_sem.at[chunks + i])
        load.start()
        small.append(load)

    barrier = pltpu.get_barrier_semaphore()
    for k in range(1, peers):
        pl.semaphore_signal(
            barrier, inc=1, device_id={"grp": lax.rem(z_me + k, peers)}, device_id_type=MESH
        )
    for k in range(1, groups):
        pl.semaphore_signal(
            barrier, inc=1, device_id={"col": lax.rem(c_me + k, groups)}, device_id_type=MESH
        )

    def remote(source, target, send, recv, axis, peer):
        return pltpu.make_async_remote_copy(
            src_ref=source,
            dst_ref=target,
            send_sem=send,
            recv_sem=recv,
            device_id={axis: peer},
            device_id_type=MESH,
        )

    def received(ref, sem):
        remote(ref, ref, sem, sem, "grp", z_me).wait_recv()

    def sent(ref, sem):
        remote(ref, ref, sem, sem, "grp", z_me).wait_send()

    def send_halos(c, b):
        rows = pl.ds(edges[b], edges[b + 1] - edges[b])
        for j in range(1, reach + 1):
            for side in range(2):
                peer = lax.rem(z_me + (peers - j if side == 0 else j), peers)
                if direct:
                    near = own if side == 0 else own + cells - DEPTH
                    far = own + cells if side == 0 else TOP
                    source = wide.at[c, :, rows, near : near + DEPTH, :]
                    target = wide.at[c, :, rows, far : far + DEPTH, :]
                else:
                    source = slabs.at[c, 2 * reach, :, rows]
                    target = slabs.at[c, 2 * (j - 1) + side, :, rows]
                remote(source, target, halo_send.at[0], halo_recv.at[c, b], "grp", peer).start()

    with jax.named_scope("barrier"):
        pl.semaphore_wait(barrier, peers - 1 + groups - 1)
    with jax.named_scope("send"):
        for c in range(chunks):
            loads[c].wait()
            for b in range(len(edges) - 1):
                send_halos(c, b)

    with jax.named_scope("forcing"):
        for load in small:
            load.wait()
        owner = jnp.concatenate(
            [owner_ref[pl.ds(c, groups, stride=chunks), :] for c in range(chunks)], axis=1
        )
        own_row = jnp.concatenate(
            [owner_ref[pl.ds(c_me * chunks + c, 1), :] for c in range(chunks)], axis=1
        )
        group_ids = lax.broadcasted_iota(jnp.int32, (groups, columns), 0)
        earlier = (
            lax.broadcasted_iota(jnp.int32, (columns, columns), 0)
            < lax.broadcasted_iota(jnp.int32, (columns, columns), 1)
        ).astype(jnp.float32)
        slot = lax.broadcasted_iota(jnp.int32, (cap, columns), 0).astype(jnp.float32)
        spot = lax.broadcasted_iota(jnp.int32, (cap, columns), 1).astype(jnp.float32) + 1.0

        def ranked(hits):
            rank = jnp.dot(hits, earlier, preferred_element_type=jnp.float32)
            return jnp.where(hits > 0.5, rank, -1.0)

        low = own_row - group_ids * columns
        order = ranked(jnp.where((low >= 0) & (low < columns), 1.0, 0.0))
        for q in range(groups):
            hot = jnp.where(order[q : q + 1] == slot, 1.0, 0.0)
            give[q * cap : (q + 1) * cap, :] = hot
        give_out = pltpu.make_async_copy(give, give_hbm, out_sem.at[0])
        give_out.start()

        for f, ref in ((0, prof_ref), (1, cour_ref)):
            lines = ref.shape[0]
            fsend[:, :, f * LANES : f * LANES + lines] = pick(
                parts_of(ref[...]), give[...].astype(jnp.bfloat16), ((1,), (1,)), swap=True
            ).reshape(groups, cap, lines)
        for k in range(1, groups):
            peer = lax.rem(c_me + k, groups)
            remote(
                fsend.at[peer], fland.at[c_me], swap_sem.at[0], swap_sem.at[1], "col", peer
            ).start()
        fland[c_me] = fsend[c_me]

        local = owner - c_me * columns
        order = ranked(jnp.where((local >= 0) & (local < columns), 1.0, 0.0))
        place = (local + 1).astype(jnp.float32)
        for q in range(groups):
            chosen = jnp.where(order[q : q + 1] == slot, place[q : q + 1], 0.0)
            chosen = jnp.sum(chosen, axis=1, keepdims=True)
            take[q * cap : (q + 1) * cap, :] = jnp.where(chosen == spot, 1.0, 0.0)
        hot = take[...].astype(jnp.bfloat16)

    with jax.named_scope("force_wait"):
        received(fland.at[pl.ds(0, groups - 1)], swap_sem.at[1])
    with jax.named_scope("force_take"):
        landed = fland[:, :, :LANES].reshape(groups * cap, LANES)
        phys = pick(parts_of(landed), hot, ((0,), (0,))) / STEPS
        landed = fland[:, :, LANES:].reshape(groups * cap, LANES)
        speed = 0.5 * pick(parts_of(landed), hot, ((0,), (0,)))
        for c in range(chunks):
            lanes = slice(c * LANES, (c + 1) * LANES)
            west = diffuse_x + speed[:levels, lanes]
            east = diffuse_x - speed[:levels, lanes]
            heat = SCALE * phys[:levels, lanes]
            rain = phys[levels : 2 * levels, lanes]
            rows = (SCALE * west, west, SCALE * east, east, heat - 1.0, rain + sat_scale, heat, rain)
            for i, row in enumerate(rows):
                coef[c, i] = row
    rain_gain = cond_rate * cloud_ref[...].astype(jnp.float32)
    heat_gain = (latent_gain * SCALE) * rain_gain

    def stepped(c, s, z):
        rows = width - 2 * s if s == STEPS else round_up(width - 2 * s, 8)
        first = TOP + (width - rows) // 2
        source = wide.at[c] if s == 1 else (odd if s % 2 == 0 else even)
        if isinstance(z, int):
            up, down = min(z + 1, levels - 1), max(z - 1, 0)
        else:
            up, down = jnp.minimum(z + 1, levels - 1), jnp.maximum(z - 1, 0)
        lanes = slice(c * LANES, (c + 1) * LANES)
        new = []
        for f in range(fields):
            scale = SCALE if s == 1 and f == 0 else 1.0
            pick_row = lambda i: coef[c, i, pl.ds(z, 1), :]
            west_gain = pick_row(0 if scale != 1.0 else 1)
            east_gain = pick_row(2 if scale != 1.0 else 3)
            push = pick_row((4 if s == 1 else 6) + f)
            here = source[f, z, first : first + rows]
            west = source[f, z, first - 1 : first - 1 + rows]
            east = source[f, z, first + 1 : first + 1 + rows]
            upper = source[f, up, first : first + rows]
            lower = source[f, down, first : first + rows]
            new.append(
                (
                    (scale * (1.0 - 2.0 * diffuse_x - 2.0 * diffuse_z)) * here
                    + (scale * diffuse_z) * (upper + lower)
                )
                + ((west_gain * west + east_gain * east) + push)
            )
        energy, moisture = new
        excess = jnp.maximum(moisture - jnp.exp2(energy), 0.0)
        energy = energy + excess * heat_gain[:, lanes]
        moisture = moisture - excess * rain_gain[:, lanes]
        if s == STEPS:
            energy = energy * (1.0 / SCALE) + 1.0 / SCALE
            moisture = moisture - sat_scale
        return first, rows, (energy, moisture)

    def put(c, s, z, result, sums, row):
        first, rows, values = result
        target = odd if s % 2 else even
        for f, value in enumerate(values):
            if s == STEPS:
                outs[f, z, :, c * LANES : (c + 1) * LANES] = value
                if direct:
                    old = wide[c, f, z, own : own + cells]
                else:
                    old = slabs[c, 2 * reach, f, z]
                sums[pl.ds(row(f, z), 1), :] = jnp.sum(value - old, axis=0, keepdims=True)
            else:
                target[f, z, first : first + rows] = value

    def sweep(c, s, low, count, sums, row, unroll):
        def body(i, carry):
            z = low + unroll * i
            results = [stepped(c, s, z + k) for k in range(unroll)]
            for k in range(unroll):
                put(c, s, z + k, results[k], sums, row)
            return carry

        trips = count // unroll
        if trips == 1:
            body(0, 0)
        elif trips > 1:
            lax.fori_loop(0, trips, body, 0)
        rest = [low + k for k in range(trips * unroll, count)]
        results = [stepped(c, s, z) for z in rest]
        for z, result in zip(rest, results):
            put(c, s, z, result, sums, row)

    def arrive(c, b, start, count):
        rows = pl.ds(start, count)
        if direct:
            received(wide.at[c, :, rows, TOP : TOP + 2 * DEPTH, :], halo_recv.at[c, b])
        else:
            received(slabs.at[c, pl.ds(0, 2 * reach), :, rows], halo_recv.at[c, b])

            def fill(z, carry):
                for f in range(fields):
                    wide[c, f, z, own : own + cells] = slabs[c, 2 * reach, f, z]
                    for j in range(1, reach + 1):
                        right = own + j * cells
                        left = own - j * cells
                        wide[c, f, z, right : right + cells] = slabs[c, 2 * j - 2, f, z]
                        wide[c, f, z, left : left + cells] = slabs[c, 2 * j - 1, f, z]
                return carry

            lax.fori_loop(start, start + count, fill, 0)

    def opening(c, sums, row):
        with jax.named_scope(f"first#c={c}"):
            arrive(c, 0, 0, BLOCK)
            for s in range(1, STEPS + 1):
                sweep(c, s, 0, BLOCK - s, sums, row, 2)

        def body(b, carry):
            with jax.named_scope("arrive"):
                arrive(c, b, b * BLOCK, BLOCK)
            with jax.named_scope("steps"):
                for s in range(1, STEPS + 1):
                    sweep(c, s, b * BLOCK - s, BLOCK, sums, row, 4)
            return carry

        lax.fori_loop(1, full, body, 0)

    def scatter(part, landing, sem):
        lines = part.shape[0] // peers
        for k in range(1, peers):
            peer = lax.rem(z_me + k, peers)
            block = pl.ds(pl.multiple_of(peer * lines, lines), lines)
            remote(part.at[block], landing.at[k - 1], sem.at[0], sem.at[1], "grp", peer).start()

    def gather(part, landing, piece, result, sem, sem2):
        lines = part.shape[0] // peers
        block = pl.ds(pl.multiple_of(z_me * lines, lines), lines)
        total = part[block, :]
        received(landing, sem.at[1])
        for k in range(peers - 1):
            total = total + landing[k]
        piece[...] = total
        result[block, :] = total
        for k in range(1, peers):
            peer = lax.rem(z_me + k, peers)
            remote(piece, result.at[block], sem2.at[0], sem2.at[1], "grp", peer).start()

    def others(ref):
        return ref.at[pl.ds(0, ref.shape[0] // peers * (peers - 1))]

    last = chunks - 1
    for c in range(last):
        whole[c, fields * levels :, :] = jnp.zeros_like(whole[c, fields * levels :, :])
        row = lambda f, z: f * levels + z
        opening(c, whole.at[c], row)
        for b in range(full, len(edges) - 1):
            arrive(c, b, edges[b], edges[b + 1] - edges[b])
        with jax.named_scope("closing"):
            for s in range(1, STEPS + 1):
                sweep(c, s, edges[full] - s, levels - edges[full] + s, whole.at[c], row, 2)
        scatter(whole.at[c], heap.at[c], sum_sem.at[2 * c])
        pltpu.make_async_copy(
            outs.at[:, :, :, span(c)], final_hbm.at[:, :, :, span(c)], out_sem.at[1]
        ).start()
    early[fields * split :, :] = jnp.zeros_like(early[fields * split :, :])
    late[fields * (levels - split) :, :] = jnp.zeros_like(late[fields * (levels - split) :, :])
    opening(last, early, lambda f, z: f * split + z)
    scatter(early, early_heap, sum_sem.at[2 * last])
    pltpu.make_async_copy(
        outs.at[:, pl.ds(0, split), :, span(last)],
        final_hbm.at[:, pl.ds(0, split), :, span(last)],
        out_sem.at[1],
    ).start()
    row = lambda f, z: f * (levels - split) + z - split
    for b in range(full, len(edges) - 1):
        with jax.named_scope(f"late_arrive#b={b}"):
            arrive(last, b, edges[b], edges[b + 1] - edges[b])
        with jax.named_scope(f"late_steps#b={b}"):
            ends = b == len(edges) - 2
            for s in range(1, STEPS + 1):
                count = edges[b + 1] - edges[b] + (s if ends else 0)
                sweep(last, s, edges[b] - s, count, late, row, count if ends else 4)
    for k in range(1, peers):
        peer = lax.rem(z_me + k, peers)
        remote(
            late, late_heap.at[k - 1], sum_sem.at[2 * last + 2, 0], sum_sem.at[2 * last + 2, 1], "grp", peer
        ).start()
    pltpu.make_async_copy(
        outs.at[:, pl.ds(split, levels - split), :, span(last)],
        final_hbm.at[:, pl.ds(split, levels - split), :, span(last)],
        out_sem.at[1],
    ).start()
    with jax.named_scope("scatter_wait"):
        for c in range(last):
            gather(whole.at[c], heap.at[c], mine.at[c], inc.at[c], sum_sem.at[2 * c], sum_sem.at[2 * c + 1])
        gather(early, early_heap, early_mine, early_inc, sum_sem.at[2 * last], sum_sem.at[2 * last + 1])
    with jax.named_scope("late_wait"):
        received(late_heap, sum_sem.at[2 * last + 2, 1])
        total = late[...]
        for k in range(peers - 1):
            total = total + late_heap[k]
        for f in range(fields):
            inc[last, f * levels + split : (f + 1) * levels, :] = total[
                f * (levels - split) : (f + 1) * (levels - split)
            ]
        inc[last, fields * levels :, :] = jnp.zeros_like(inc[last, fields * levels :, :])
    with jax.named_scope("gather_wait"):
        packed = 0.0
        for c in range(last):
            received(others(inc.at[c]), sum_sem.at[2 * c + 1, 1])
            packed = packed + pick(
                parts_of(inc[c]), hot[:, c * LANES : (c + 1) * LANES], ((1,), (1,)), swap=True
            )
        received(others(early_inc), sum_sem.at[2 * last + 1, 1])
    with jax.named_scope("pack"):
        for f in range(fields):
            inc[last, f * levels : f * levels + split, :] = early_inc[f * split : (f + 1) * split, :]
        packed = packed + pick(
            parts_of(inc[last]), hot[:, last * LANES :], ((1,), (1,)), swap=True
        )
        pack[...] = (packed / (cells * peers)).reshape(pack.shape)
    for k in range(1, groups):
        peer = lax.rem(c_me + k, groups)
        remote(pack.at[peer], land.at[c_me], swap_sem.at[2], swap_sem.at[3], "col", peer).start()
    keep = pltpu.make_async_copy(pack.at[c_me], land.at[c_me], out_sem.at[2])
    keep.start()
    with jax.named_scope("drain"):
        if direct:
            sent(wide.at[:, :, :, TOP : TOP + 2 * DEPTH, :], halo_send.at[0])
        else:
            sent(slabs.at[:, pl.ds(0, 2 * reach)], halo_send.at[0])
        sent(fsend.at[pl.ds(0, groups - 1)], swap_sem.at[0])
        for c in range(last):
            sent(others(inc.at[c]), sum_sem.at[2 * c, 0])
            sent(others(inc.at[c]), sum_sem.at[2 * c + 1, 0])
        sent(others(early_inc), sum_sem.at[2 * last, 0])
        sent(others(early_inc), sum_sem.at[2 * last + 1, 0])
        sent(late_heap, sum_sem.at[2 * last + 2, 0])
        give_out.wait()
        pltpu.make_async_copy(outs, final_hbm, out_sem.at[1]).wait()
        keep.wait()
        sent(pack.at[pl.ds(0, groups - 1)], swap_sem.at[2])
    with jax.named_scope("return_wait"):
        received(land.at[pl.ds(0, groups - 1)], swap_sem.at[3])


def finish_kernel(
    land_hbm, give_hbm, state_hbm, tend_hbm, final_hbm, land, give, state, tend, in_sem, out_sem
):
    fields, levels = state.shape[:2]
    groups, cap, rows = land.shape
    small = [
        pltpu.make_async_copy(land_hbm, land, in_sem.at[0]),
        pltpu.make_async_copy(give_hbm, give, in_sem.at[1]),
    ]
    half = levels // 2
    pieces = [(f, pl.ds(i * half, half + i * (levels % 2))) for f in range(fields) for i in range(2)]
    ins = [
        pltpu.make_async_copy(state_hbm.at[f, z], state.at[f, z], in_sem.at[2 + i])
        for i, (f, z) in enumerate(pieces)
    ]
    stores = [
        pltpu.make_async_copy(state.at[f, z], final_hbm.at[f, z], out_sem.at[i])
        for i, (f, z) in enumerate(pieces)
    ]
    for copy in small + ins:
        copy.start()
    for copy in small:
        copy.wait()
    split = parts_of(land[...].reshape(groups * cap, rows))
    hot = give[...].astype(jnp.bfloat16)
    for load, store in zip(ins, stores):
        load.wait()
        store.start()
    back = pick(split, hot, ((0,), (0,)))
    tend[...] = back[: tend.shape[0]]
    store = pltpu.make_async_copy(tend, tend_hbm, out_sem.at[len(pieces)])
    store.start()
    for copy in stores + [store]:
        copy.wait()


def on_device(profiles, courant, owner_map, cloud_flags, crm_state):
    columns = profiles.shape[0]
    fields, levels, cells = crm_state.shape[:3]
    groups = lax.axis_size("col")
    peers = lax.axis_size("grp")
    per_peer = columns // groups
    cap = round_up(per_peer + min(2, per_peer), 8)
    chunks = columns // LANES
    direct = cells % 8 == 0
    reach = 1 if direct else DEPTH // cells
    full, edges = level_edges(levels)
    split = (full - 1) * BLOCK
    rows = round_up(fields * levels, 8 * peers)
    early_rows = round_up(fields * split, 8 * peers)
    late_rows = round_up(fields * (levels - split), 8)
    f32 = lambda *shape: pltpu.VMEM(shape, jnp.float32)
    i32 = lambda *shape: pltpu.VMEM(shape, jnp.int32)
    dma = lambda *shape: pltpu.SemaphoreType.DMA(shape)
    anywhere = pl.BlockSpec(memory_space=pl.ANY)
    tall = round_up(TOP + cells + 2 * DEPTH + 1, 8)
    slabs = (8, 128) if direct else (chunks, 2 * reach + 1, fields, levels, cells, LANES)
    land, give, state = pl.pallas_call(
        window_kernel,
        out_shape=(
            jax.ShapeDtypeStruct((groups, cap, rows), jnp.float32),
            jax.ShapeDtypeStruct((groups * cap, columns), jnp.float32),
            jax.ShapeDtypeStruct(crm_state.shape, jnp.float32),
        ),
        in_specs=[anywhere] * 5,
        out_specs=(anywhere,) * 3,
        scratch_shapes=[
            f32(fields * levels, columns),
            f32(levels, columns),
            i32(groups * chunks, LANES),
            i32(1, columns),
            f32(chunks, fields, levels, tall, LANES),
            f32(*slabs),
            f32(fields, levels, tall, LANES),
            f32(fields, levels, tall, LANES),
            f32(fields, levels, cells, columns),
            f32(groups * cap, columns),
            f32(groups * cap, columns),
            f32(groups, cap, 2 * LANES),
            f32(groups, cap, 2 * LANES),
            f32(chunks, 8, levels, LANES),
            f32(chunks, rows, LANES),
            f32(early_rows, LANES),
            f32(late_rows, LANES),
            f32(chunks, peers - 1, rows // peers, LANES),
            f32(peers - 1, early_rows // peers, LANES),
            f32(peers - 1, late_rows, LANES),
            f32(chunks, rows // peers, LANES),
            f32(early_rows // peers, LANES),
            f32(chunks, rows, LANES),
            f32(early_rows, LANES),
            f32(groups, cap, rows),
            dma(chunks + 4),
            dma(3),
            dma(1),
            dma(chunks, len(edges) - 1),
            dma(4),
            dma(2 * chunks + 1, 2),
        ],
        compiler_params=pltpu.CompilerParams(
            collective_id=0, has_side_effects=True, vmem_limit_bytes=LIMIT
        ),
    )(
        profiles.T,
        courant.T,
        owner_map.reshape(groups * chunks, LANES),
        cloud_flags[None, :],
        crm_state,
    )
    tendency, final = pl.pallas_call(
        finish_kernel,
        out_shape=(
            jax.ShapeDtypeStruct((fields * levels, columns), jnp.float32),
            jax.ShapeDtypeStruct(crm_state.shape, jnp.float32),
        ),
        in_specs=[anywhere] * 3,
        out_specs=(anywhere,) * 2,
        scratch_shapes=[
            f32(groups, cap, rows),
            f32(groups * cap, columns),
            f32(*crm_state.shape),
            f32(fields * levels, columns),
            dma(2 + 2 * fields),
            dma(1 + 2 * fields),
        ],
        compiler_params=pltpu.CompilerParams(vmem_limit_bytes=LIMIT),
    )(land, give, state)
    return tendency.T, final


def solution(mesh):
    placed = (P("col", None), P("col", None), P(), P("col"), P(None, None, "grp", "col"))
    return jax.shard_map(
        on_device,
        mesh=mesh,
        in_specs=placed,
        out_specs=(P("col", None), P(None, None, "grp", "col")),
        check_vma=False,
    )
```

```python
import jax
import jax.numpy as jnp
from jax import lax
from jax.experimental import pallas as pl
from jax.experimental.pallas import tpu as pltpu
from jax.sharding import PartitionSpec as P

STEPS = 8
DEPTH = STEPS
BLOCK = 8
PIECE = 4
AHEAD = 3
LEAD = 3
HELD = -1
PIECES = 2
LANES = 128
LIMIT = 67_043_328
TOP = 8
MESH = pl.DeviceIdType.MESH

diffuse_x = 0.25
diffuse_z = 0.2
sat_scale = 0.5
sat_slope = 0.3
cond_rate = 0.5
latent_gain = 0.4
SCALE = sat_slope * 1.4426950408889634


def round_up(n, m):
    return -(-n // m) * m


def parts_of(x):
    high = x.astype(jnp.bfloat16)
    rest = x - high.astype(jnp.float32)
    middle = rest.astype(jnp.bfloat16)
    return high, middle, (rest - middle.astype(jnp.float32)).astype(jnp.bfloat16)


def pick(parts, hot, dims, swap=False):
    total = 0.0
    for part in parts:
        pair = (hot, part) if swap else (part, hot)
        total = total + lax.dot_general(
            *pair, (dims, ((), ())), preferred_element_type=jnp.float32
        )
    return total


def flip(index, mask):
    place = index
    for i in range(mask.bit_length()):
        if mask >> i & 1:
            place = place + (1 << i) - (2 << i) * lax.rem(lax.div(index, 1 << i), 2)
    return place


def level_edges(levels):
    full = max(2, (levels - BLOCK) // BLOCK)
    edges = [i * BLOCK for i in range(full + 1)]
    while edges[-1] < levels:
        edges.append(min(edges[-1] + PIECE, levels))
    return full, edges


def window_kernel(
    prof_hbm,
    cour_hbm,
    owner_hbm,
    cloud_hbm,
    x_hbm,
    land,
    give_hbm,
    final_hbm,
    prof_ref,
    cour_ref,
    owner_ref,
    cloud_ref,
    wide,
    slabs,
    odd,
    even,
    outs,
    give,
    take,
    fsend,
    fland,
    coef,
    whole,
    early,
    late,
    heap,
    early_heap,
    late_heap,
    mine,
    early_mine,
    inc,
    early_inc,
    pack,
    load_sem,
    out_sem,
    halo_send,
    halo_recv,
    swap_sem,
    sum_sem,
    meet,
):
    fields, levels, cells, columns = x_hbm.shape
    chunks = columns // LANES
    groups, cap = fland.shape[:2]
    peers = lax.axis_size("grp")
    z_me = lax.axis_index("grp")
    c_me = lax.axis_index("col")
    direct = cells % 8 == 0
    reach = 1 if direct else DEPTH // cells
    width = cells + 2 * DEPTH
    own = TOP + DEPTH
    full, edges = level_edges(levels)
    split = edges[full + HELD] - BLOCK
    span = lambda i: pl.ds(i * LANES, LANES)

    loads = []
    for c in range(chunks):
        if direct:
            target = wide.at[c, :, :, own : own + cells, :]
        else:
            target = slabs.at[c, 2 * reach]
        load = pltpu.make_async_copy(x_hbm.at[:, :, :, span(c)], target, load_sem.at[c])
        load.start()
        loads.append(load)
    small = []
    pairs = ((prof_hbm, prof_ref), (cour_hbm, cour_ref), (owner_hbm, owner_ref), (cloud_hbm, cloud_ref))
    for i, (source, target) in enumerate(pairs):
        load = pltpu.make_async_copy(source, target, load_sem.at[chunks + i])
        load.start()
        small.append(load)

    def remote(source, target, send, recv, axis, peer):
        return pltpu.make_async_remote_copy(
            src_ref=source,
            dst_ref=target,
            send_sem=send,
            recv_sem=recv,
            device_id={axis: peer},
            device_id_type=MESH,
        )

    def received(ref, sem):
        remote(ref, ref, sem, sem, "grp", z_me).wait_recv()

    def sent(ref, sem):
        remote(ref, ref, sem, sem, "grp", z_me).wait_send()

    def send_slabs(c, b):
        rows = pl.ds(edges[b], edges[b + 1] - edges[b])
        for j in range(1, reach + 1):
            for side in range(2):
                peer = lax.rem(z_me + (peers - j if side == 0 else j), peers)
                source = slabs.at[c, 2 * reach, :, rows]
                target = slabs.at[c, 2 * (j - 1) + side, :, rows]
                remote(source, target, halo_send.at[0], halo_recv.at[c, b], "grp", peer).start()

    lead = jnp.where(z_me == peers - 1, 1, 0)
    items = [(c, b) for c in range(chunks) for b in range(len(edges) - 1)]

    def send_rows(i, side):
        c, b = items[i]
        rows = pl.ds(edges[b], edges[b + 1] - edges[b])
        peer = lax.rem(z_me + side + (1 - side) * (peers - 1), peers)
        near = pl.multiple_of(own + side * (cells - DEPTH), 8)
        far = pl.multiple_of(own + cells - side * (cells + DEPTH), 8)
        source = wide.at[c, :, rows, pl.ds(near, DEPTH), :]
        target = wide.at[c, :, rows, pl.ds(far, DEPTH), :]
        remote(source, target, halo_send.at[0], halo_recv.at[c, b], "grp", peer).start()

    barrier = pltpu.get_barrier_semaphore()

    def signal(sem, axis, peer):
        pl.semaphore_signal(sem, inc=1, device_id={axis: peer}, device_id_type=MESH)

    if direct and peers > 2 and groups & (groups - 1) == 0:
        at_left, at_right = z_me == 0, z_me == peers - 1
        ends = at_left | at_right
        bits = [1 << i for i in range(groups.bit_length() - 1)]
        across = [flip(c_me, k) for k in bits]

        @pl.when(z_me > 0)
        def _():
            signal(barrier, "grp", z_me - 1)

        @pl.when(z_me < peers - 1)
        def _():
            signal(barrier, "grp", z_me + 1)

        for peer in across:
            signal(barrier, "col", peer)
        with jax.named_scope("barrier"):
            pl.semaphore_wait(barrier, len(bits) + 2 - jnp.where(ends, 1, 0))
        with jax.named_scope("send"):
            loads[0].wait()
            for i in range(AHEAD):
                send_rows(i, 1 - lead)

            @pl.when(jnp.logical_not(ends))
            def _():
                for i in range(AHEAD):
                    send_rows(i, lead)

            @pl.when((z_me > 0) & (z_me < peers - 1))
            def _():
                signal(meet.at[0], "grp", z_me - 1)
                signal(meet.at[1], "grp", z_me + 1)

            for r in range(peers - 2):

                @pl.when(r < peers - 2 - z_me)
                def _():
                    pl.semaphore_wait(meet.at[0], 1)

                    @pl.when(z_me > 0)
                    def _():
                        signal(meet.at[0], "grp", z_me - 1)

                @pl.when(r < z_me - 1)
                def _():
                    pl.semaphore_wait(meet.at[1], 1)

                    @pl.when(z_me < peers - 1)
                    def _():
                        signal(meet.at[1], "grp", z_me + 1)

            @pl.when(ends)
            def _():
                for i in range(AHEAD):
                    send_rows(i, lead)

            for load in loads[1:]:
                load.wait()
            for i in range(AHEAD, AHEAD + LEAD):
                send_rows(i, lead)
            for i in range(AHEAD, len(items)):
                send_rows(i, 1 - lead)
                if i + LEAD < len(items):
                    send_rows(i + LEAD, lead)
            for i, peer in enumerate(across[1:]):
                signal(meet.at[2 + i], "col", peer)
                pl.semaphore_wait(meet.at[2 + i], 1)
    else:
        for k in range(1, peers):
            signal(barrier, "grp", lax.rem(z_me + k, peers))
        for k in range(1, groups):
            signal(barrier, "col", lax.rem(c_me + k, groups))
        pl.semaphore_wait(barrier, peers - 1 + groups - 1)
        for load in loads:
            load.wait()
        for i, (c, b) in enumerate(items):
            if direct:
                send_rows(i, 0)
                send_rows(i, 1)
            else:
                send_slabs(c, b)

    with jax.named_scope("forcing"):
        for load in small:
            load.wait()
        owner = jnp.concatenate(
            [owner_ref[pl.ds(c, groups, stride=chunks), :] for c in range(chunks)], axis=1
        )
        own_row = jnp.concatenate(
            [owner_ref[pl.ds(c_me * chunks + c, 1), :] for c in range(chunks)], axis=1
        )
        group_ids = lax.broadcasted_iota(jnp.int32, (groups, columns), 0)
        earlier = (
            lax.broadcasted_iota(jnp.int32, (columns, columns), 0)
            < lax.broadcasted_iota(jnp.int32, (columns, columns), 1)
        ).astype(jnp.float32)
        slot = lax.broadcasted_iota(jnp.int32, (cap, columns), 0).astype(jnp.float32)
        spot = lax.broadcasted_iota(jnp.int32, (cap, columns), 1).astype(jnp.float32) + 1.0

        def ranked(hits):
            rank = jnp.dot(hits, earlier, preferred_element_type=jnp.float32)
            return jnp.where(hits > 0.5, rank, -1.0)

        low = own_row - group_ids * columns
        order = ranked(jnp.where((low >= 0) & (low < columns), 1.0, 0.0))
        for q in range(groups):
            hot = jnp.where(order[q : q + 1] == slot, 1.0, 0.0)
            give[q * cap : (q + 1) * cap, :] = hot
        give_out = pltpu.make_async_copy(give, give_hbm, out_sem.at[0])
        give_out.start()

        for f, ref in ((0, prof_ref), (1, cour_ref)):
            lines = ref.shape[0]
            fsend[:, :, f * LANES : f * LANES + lines] = pick(
                parts_of(ref[...]), give[...].astype(jnp.bfloat16), ((1,), (1,)), swap=True
            ).reshape(groups, cap, lines)
        for k in range(1, groups):
            peer = lax.rem(c_me + k, groups)
            remote(
                fsend.at[peer], fland.at[c_me], swap_sem.at[0], swap_sem.at[1], "col", peer
            ).start()
        fland[c_me] = fsend[c_me]

        local = owner - c_me * columns
        order = ranked(jnp.where((local >= 0) & (local < columns), 1.0, 0.0))
        place = (local + 1).astype(jnp.float32)
        for q in range(groups):
            chosen = jnp.where(order[q : q + 1] == slot, place[q : q + 1], 0.0)
            chosen = jnp.sum(chosen, axis=1, keepdims=True)
            take[q * cap : (q + 1) * cap, :] = jnp.where(chosen == spot, 1.0, 0.0)
        hot = take[...].astype(jnp.bfloat16)

    with jax.named_scope("force_wait"):
        received(fland.at[pl.ds(0, groups - 1)], swap_sem.at[1])
    with jax.named_scope("force_take"):
        landed = fland[:, :, :LANES].reshape(groups * cap, LANES)
        phys = pick(parts_of(landed), hot, ((0,), (0,))) / STEPS
        landed = fland[:, :, LANES:].reshape(groups * cap, LANES)
        speed = 0.5 * pick(parts_of(landed), hot, ((0,), (0,)))
        for c in range(chunks):
            lanes = slice(c * LANES, (c + 1) * LANES)
            west = diffuse_x + speed[:levels, lanes]
            east = diffuse_x - speed[:levels, lanes]
            heat = SCALE * phys[:levels, lanes]
            rain = phys[levels : 2 * levels, lanes]
            rows = (SCALE * west, west, SCALE * east, east, heat - 1.0, rain + sat_scale, heat, rain)
            for i, row in enumerate(rows):
                coef[c, i] = row
    rain_gain = cond_rate * cloud_ref[...].astype(jnp.float32)
    heat_gain = (latent_gain * SCALE) * rain_gain

    def stepped(c, s, z):
        rows = width - 2 * s if s == STEPS else round_up(width - 2 * s, 8)
        first = TOP + (width - rows) // 2
        source = wide.at[c] if s == 1 else (odd if s % 2 == 0 else even)
        if isinstance(z, int):
            up, down = min(z + 1, levels - 1), max(z - 1, 0)
        else:
            up, down = jnp.minimum(z + 1, levels - 1), jnp.maximum(z - 1, 0)
        lanes = slice(c * LANES, (c + 1) * LANES)
        new = []
        for f in range(fields):
            scale = SCALE if s == 1 and f == 0 else 1.0
            pick_row = lambda i: coef[c, i, pl.ds(z, 1), :]
            west_gain = pick_row(0 if scale != 1.0 else 1)
            east_gain = pick_row(2 if scale != 1.0 else 3)
            push = pick_row((4 if s == 1 else 6) + f)
            here = source[f, z, first : first + rows]
            west = source[f, z, first - 1 : first - 1 + rows]
            east = source[f, z, first + 1 : first + 1 + rows]
            upper = source[f, up, first : first + rows]
            lower = source[f, down, first : first + rows]
            new.append(
                (
                    (scale * (1.0 - 2.0 * diffuse_x - 2.0 * diffuse_z)) * here
                    + (scale * diffuse_z) * (upper + lower)
                )
                + ((west_gain * west + east_gain * east) + push)
            )
        energy, moisture = new
        excess = jnp.maximum(moisture - jnp.exp2(energy), 0.0)
        energy = energy + excess * heat_gain[:, lanes]
        moisture = moisture - excess * rain_gain[:, lanes]
        if s == STEPS:
            energy = energy * (1.0 / SCALE) + 1.0 / SCALE
            moisture = moisture - sat_scale
        return first, rows, (energy, moisture)

    def put(c, s, z, result, sums, row):
        first, rows, values = result
        target = odd if s % 2 else even
        for f, value in enumerate(values):
            if s == STEPS:
                outs[f, z, :, c * LANES : (c + 1) * LANES] = value
                if direct:
                    old = wide[c, f, z, own : own + cells]
                else:
                    old = slabs[c, 2 * reach, f, z]
                sums[pl.ds(row(f, z), 1), :] = jnp.sum(value - old, axis=0, keepdims=True)
            else:
                target[f, z, first : first + rows] = value

    def sweep(c, s, low, count, sums, row, unroll):
        def body(i, carry):
            z = low + unroll * i
            results = [stepped(c, s, z + k) for k in range(unroll)]
            for k in range(unroll):
                put(c, s, z + k, results[k], sums, row)
            return carry

        trips = count // unroll
        if trips == 1:
            body(0, 0)
        elif trips > 1:
            lax.fori_loop(0, trips, body, 0)
        rest = [low + k for k in range(trips * unroll, count)]
        results = [stepped(c, s, z) for z in rest]
        for z, result in zip(rest, results):
            put(c, s, z, result, sums, row)

    def arrive(c, b, start, count):
        rows = pl.ds(start, count)
        if direct:
            received(wide.at[c, :, rows, TOP : TOP + 2 * DEPTH, :], halo_recv.at[c, b])
        else:
            received(slabs.at[c, pl.ds(0, 2 * reach), :, rows], halo_recv.at[c, b])

            def fill(z, carry):
                for f in range(fields):
                    wide[c, f, z, own : own + cells] = slabs[c, 2 * reach, f, z]
                    for j in range(1, reach + 1):
                        right = own + j * cells
                        left = own - j * cells
                        wide[c, f, z, right : right + cells] = slabs[c, 2 * j - 2, f, z]
                        wide[c, f, z, left : left + cells] = slabs[c, 2 * j - 1, f, z]
                return carry

            lax.fori_loop(start, start + count, fill, 0)

    def opening(c, sums, row, stop):
        with jax.named_scope(f"first#c={c}"):
            arrive(c, 0, 0, BLOCK)
            for s in range(1, STEPS + 1):
                sweep(c, s, 0, BLOCK - s, sums, row, 2)

        def body(b, carry):
            with jax.named_scope("arrive"):
                arrive(c, b, b * BLOCK, BLOCK)
            with jax.named_scope("steps"):
                for s in range(1, STEPS + 1):
                    sweep(c, s, b * BLOCK - s, BLOCK, sums, row, 4)
            return carry

        lax.fori_loop(1, stop, body, 0)

    def scatter(part, landing, sem):
        lines = part.shape[0] // peers
        for k in range(1, peers):
            peer = lax.rem(z_me + k, peers)
            block = pl.ds(pl.multiple_of(peer * lines, lines), lines)
            remote(part.at[block], landing.at[k - 1], sem.at[0], sem.at[1], "grp", peer).start()

    def gather(part, landing, piece, result, sem, sem2):
        lines = part.shape[0] // peers
        block = pl.ds(pl.multiple_of(z_me * lines, lines), lines)
        total = part[block, :]
        received(landing, sem.at[1])
        for k in range(peers - 1):
            total = total + landing[k]
        piece[...] = total
        result[block, :] = total
        for k in range(1, peers):
            peer = lax.rem(z_me + k, peers)
            remote(piece, result.at[block], sem2.at[0], sem2.at[1], "grp", peer).start()

    def others(ref):
        return ref.at[pl.ds(0, ref.shape[0] // peers * (peers - 1))]

    last = chunks - 1
    for c in range(last):
        whole[c, fields * levels :, :] = jnp.zeros_like(whole[c, fields * levels :, :])
        row = lambda f, z: f * levels + z
        opening(c, whole.at[c], row, full)
        for b in range(full, len(edges) - 1):
            arrive(c, b, edges[b], edges[b + 1] - edges[b])
        with jax.named_scope("closing"):
            for s in range(1, STEPS + 1):
                sweep(c, s, edges[full] - s, levels - edges[full] + s, whole.at[c], row, 2)
        scatter(whole.at[c], heap.at[c], sum_sem.at[2 * c])
        pltpu.make_async_copy(
            outs.at[:, :, :, span(c)], final_hbm.at[:, :, :, span(c)], out_sem.at[1]
        ).start()
    if early.shape[0] > fields * split:
        early[fields * split :, :] = jnp.zeros_like(early[fields * split :, :])
    if late.shape[0] > fields * (levels - split):
        late[fields * (levels - split) :, :] = jnp.zeros_like(late[fields * (levels - split) :, :])
    early_row = lambda f, z: f * split + z
    late_row = lambda f, z: f * (levels - split) + z - split
    pause = full + min(HELD, 0)
    opening(last, early, early_row, pause)
    for b in range(pause, len(edges) - 1):
        if b == full + HELD:
            scatter(early, early_heap, sum_sem.at[2 * last])
            pltpu.make_async_copy(
                outs.at[:, pl.ds(0, split), :, span(last)],
                final_hbm.at[:, pl.ds(0, split), :, span(last)],
                out_sem.at[1],
            ).start()
        with jax.named_scope(f"late_arrive#b={b}"):
            arrive(last, b, edges[b], edges[b + 1] - edges[b])
        with jax.named_scope(f"late_steps#b={b}"):
            ends = b == len(edges) - 2
            sums, row = (early, early_row) if b < full + HELD else (late, late_row)
            for s in range(1, STEPS + 1):
                count = edges[b + 1] - edges[b] + (s if ends else 0)
                sweep(last, s, edges[b] - s, count, sums, row, count if ends else 4)
    late_sem = sum_sem.at[2 * chunks]
    for k in range(1, peers):
        remote(late, late_heap.at[k - 1], late_sem.at[0], late_sem.at[1], "grp", flip(z_me, k)).start()
    pltpu.make_async_copy(
        outs.at[:, pl.ds(split, levels - split), :, span(last)],
        final_hbm.at[:, pl.ds(split, levels - split), :, span(last)],
        out_sem.at[1],
    ).start()
    with jax.named_scope("scatter_wait"):
        for c in range(last):
            gather(whole.at[c], heap.at[c], mine.at[c], inc.at[c], sum_sem.at[2 * c], sum_sem.at[2 * c + 1])
        gather(early, early_heap, early_mine, early_inc, sum_sem.at[2 * last], sum_sem.at[2 * last + 1])
    with jax.named_scope("late_wait"):
        received(late_heap, late_sem.at[1])
        totals = [late[...]] + [late_heap[k] for k in range(peers - 1)]
        while len(totals) > 1:
            totals = [x + y for x, y in zip(totals[::2], totals[1::2])]
        for f in range(fields):
            inc[last, f * levels + split : (f + 1) * levels, :] = totals[0][
                f * (levels - split) : (f + 1) * (levels - split)
            ]
        inc[last, fields * levels :, :] = jnp.zeros_like(inc[last, fields * levels :, :])
    with jax.named_scope("gather_wait"):
        packed = 0.0
        for c in range(last):
            received(others(inc.at[c]), sum_sem.at[2 * c + 1, 1])
            packed = packed + pick(
                parts_of(inc[c]), hot[:, c * LANES : (c + 1) * LANES], ((1,), (1,)), swap=True
            )
        received(others(early_inc), sum_sem.at[2 * last + 1, 1])
    with jax.named_scope("pack"):
        for f in range(fields):
            inc[last, f * levels : f * levels + split, :] = early_inc[f * split : (f + 1) * split, :]
        packed = packed + pick(
            parts_of(inc[last]), hot[:, last * LANES :], ((1,), (1,)), swap=True
        )
        pack[...] = (packed / (cells * peers)).reshape(pack.shape)
    for k in sorted(range(1, groups), key=lambda k: -bin(k >> 1).count("1")):
        peer = flip(c_me, k)
        remote(pack.at[peer], land.at[c_me], swap_sem.at[2], swap_sem.at[3], "col", peer).start()
    keep = pltpu.make_async_copy(pack.at[c_me], land.at[c_me], out_sem.at[2])
    keep.start()
    with jax.named_scope("drain"):
        if direct:
            sent(wide.at[:, :, :, TOP : TOP + 2 * DEPTH, :], halo_send.at[0])
        else:
            sent(slabs.at[:, pl.ds(0, 2 * reach)], halo_send.at[0])
        sent(fsend.at[pl.ds(0, groups - 1)], swap_sem.at[0])
        for c in range(last):
            sent(others(inc.at[c]), sum_sem.at[2 * c, 0])
            sent(others(inc.at[c]), sum_sem.at[2 * c + 1, 0])
        sent(others(early_inc), sum_sem.at[2 * last, 0])
        sent(others(early_inc), sum_sem.at[2 * last + 1, 0])
        sent(late_heap, late_sem.at[0])
        give_out.wait()
        pltpu.make_async_copy(outs, final_hbm, out_sem.at[1]).wait()
        keep.wait()
        sent(pack.at[pl.ds(0, groups - 1)], swap_sem.at[2])
    with jax.named_scope("return_wait"):
        received(land.at[pl.ds(0, groups - 1)], swap_sem.at[3])


def finish_kernel(
    land_hbm, give_hbm, state_hbm, tend_hbm, final_hbm, land, give, state, tend, in_sem, out_sem
):
    fields, levels = state.shape[:2]
    groups, cap, rows = land.shape
    small = [
        pltpu.make_async_copy(land_hbm, land, in_sem.at[0]),
        pltpu.make_async_copy(give_hbm, give, in_sem.at[1]),
    ]
    cuts = [levels * i // PIECES for i in range(PIECES + 1)]
    pieces = [(f, pl.ds(a, b - a)) for f in range(fields) for a, b in zip(cuts, cuts[1:])]
    ins = [
        pltpu.make_async_copy(state_hbm.at[f, z], state.at[f, z], in_sem.at[2 + i])
        for i, (f, z) in enumerate(pieces)
    ]
    stores = [
        pltpu.make_async_copy(state.at[f, z], final_hbm.at[f, z], out_sem.at[i])
        for i, (f, z) in enumerate(pieces)
    ]
    for copy in small + ins:
        copy.start()
    for copy in small:
        copy.wait()
    split = parts_of(land[...].reshape(groups * cap, rows))
    hot = give[...].astype(jnp.bfloat16)
    for load, store in zip(ins, stores):
        load.wait()
        store.start()
    back = pick(split, hot, ((0,), (0,)))
    tend[...] = back[: tend.shape[0]]
    store = pltpu.make_async_copy(tend, tend_hbm, out_sem.at[len(pieces)])
    store.start()
    for copy in stores + [store]:
        copy.wait()


def on_device(profiles, courant, owner_map, cloud_flags, crm_state):
    columns = profiles.shape[0]
    fields, levels, cells = crm_state.shape[:3]
    groups = lax.axis_size("col")
    peers = lax.axis_size("grp")
    per_peer = columns // groups
    cap = round_up(per_peer + min(2, per_peer), 8)
    chunks = columns // LANES
    direct = cells % 8 == 0
    reach = 1 if direct else DEPTH // cells
    full, edges = level_edges(levels)
    split = edges[full + HELD] - BLOCK
    rows = round_up(fields * levels, 8 * peers)
    early_rows = round_up(fields * split, 8 * peers)
    late_rows = round_up(fields * (levels - split), 8)
    f32 = lambda *shape: pltpu.VMEM(shape, jnp.float32)
    i32 = lambda *shape: pltpu.VMEM(shape, jnp.int32)
    dma = lambda *shape: pltpu.SemaphoreType.DMA(shape)
    anywhere = pl.BlockSpec(memory_space=pl.ANY)
    tall = round_up(TOP + cells + 2 * DEPTH + 1, 8)
    slabs = (8, 128) if direct else (chunks, 2 * reach + 1, fields, levels, cells, LANES)
    land, give, state = pl.pallas_call(
        window_kernel,
        out_shape=(
            jax.ShapeDtypeStruct((groups, cap, rows), jnp.float32),
            jax.ShapeDtypeStruct((groups * cap, columns), jnp.float32),
            jax.ShapeDtypeStruct(crm_state.shape, jnp.float32),
        ),
        in_specs=[anywhere] * 5,
        out_specs=(anywhere,) * 3,
        scratch_shapes=[
            f32(fields * levels, columns),
            f32(levels, columns),
            i32(groups * chunks, LANES),
            i32(1, columns),
            f32(chunks, fields, levels, tall, LANES),
            f32(*slabs),
            f32(fields, levels, tall, LANES),
            f32(fields, levels, tall, LANES),
            f32(fields, levels, cells, columns),
            f32(groups * cap, columns),
            f32(groups * cap, columns),
            f32(groups, cap, 2 * LANES),
            f32(groups, cap, 2 * LANES),
            f32(chunks, 8, levels, LANES),
            f32(chunks, rows, LANES),
            f32(early_rows, LANES),
            f32(late_rows, LANES),
            f32(chunks, peers - 1, rows // peers, LANES),
            f32(peers - 1, early_rows // peers, LANES),
            f32(peers - 1, late_rows, LANES),
            f32(chunks, rows // peers, LANES),
            f32(early_rows // peers, LANES),
            f32(chunks, rows, LANES),
            f32(early_rows, LANES),
            f32(groups, cap, rows),
            dma(chunks + 4),
            dma(3),
            dma(1),
            dma(chunks, len(edges) - 1),
            dma(4),
            dma(2 * chunks + 1, 2),
            pltpu.SemaphoreType.REGULAR((max(2, groups.bit_length()),)),
        ],
        compiler_params=pltpu.CompilerParams(
            collective_id=0, has_side_effects=True, vmem_limit_bytes=LIMIT
        ),
    )(
        profiles.T,
        courant.T,
        owner_map.reshape(groups * chunks, LANES),
        cloud_flags[None, :],
        crm_state,
    )
    tendency, final = pl.pallas_call(
        finish_kernel,
        out_shape=(
            jax.ShapeDtypeStruct((fields * levels, columns), jnp.float32),
            jax.ShapeDtypeStruct(crm_state.shape, jnp.float32),
        ),
        in_specs=[anywhere] * 3,
        out_specs=(anywhere,) * 2,
        scratch_shapes=[
            f32(groups, cap, rows),
            f32(groups * cap, columns),
            f32(*crm_state.shape),
            f32(fields * levels, columns),
            dma(2 + PIECES * fields),
            dma(1 + PIECES * fields),
        ],
        compiler_params=pltpu.CompilerParams(vmem_limit_bytes=LIMIT),
    )(land, give, state)
    return tendency.T, final


def solution(mesh):
    placed = (P("col", None), P("col", None), P(), P("col"), P(None, None, "grp", "col"))
    return jax.shard_map(
        on_device,
        mesh=mesh,
        in_specs=placed,
        out_specs=(P("col", None), P(None, None, "grp", "col")),
        check_vma=False,
    )
```

```python
import jax
import jax.numpy as jnp
from jax import lax
from jax.experimental import pallas as pl
from jax.experimental.pallas import tpu as pltpu
from jax.sharding import PartitionSpec as P

STEPS = 8
DEPTH = STEPS
BLOCK = 8
PIECE = 4
AHEAD = 2
LEAD = 1
PIECES = 2
LANES = 128
LIMIT = 67_043_328
TOP = 8
MESH = pl.DeviceIdType.MESH

diffuse_x = 0.25
diffuse_z = 0.2
sat_scale = 0.5
sat_slope = 0.3
cond_rate = 0.5
latent_gain = 0.4
SCALE = sat_slope * 1.4426950408889634


def round_up(n, m):
    return -(-n // m) * m


def parts_of(x):
    high = x.astype(jnp.bfloat16)
    rest = x - high.astype(jnp.float32)
    middle = rest.astype(jnp.bfloat16)
    return high, middle, (rest - middle.astype(jnp.float32)).astype(jnp.bfloat16)


def pick(parts, hot, dims, swap=False):
    total = 0.0
    for part in parts:
        pair = (hot, part) if swap else (part, hot)
        total = total + lax.dot_general(
            *pair, (dims, ((), ())), preferred_element_type=jnp.float32
        )
    return total


def split_level(fields, levels, chunks, peers, limit):
    for split in range(limit, 0, -1):
        if fields * (levels * (chunks - 1) + split) % (8 * peers) == 0:
            return split
    return limit


def flip(index, mask):
    place = index
    for i in range(mask.bit_length()):
        if mask >> i & 1:
            place = place + (1 << i) - (2 << i) * lax.rem(lax.div(index, 1 << i), 2)
    return place


def level_edges(levels):
    full = max(2, (levels - BLOCK) // BLOCK)
    edges = [i * BLOCK for i in range(full + 1)]
    while edges[-1] < levels:
        edges.append(min(edges[-1] + PIECE, levels))
    return full, edges


def window_kernel(
    prof_hbm,
    cour_hbm,
    owner_hbm,
    cloud_hbm,
    x_hbm,
    land,
    give_hbm,
    final_hbm,
    prof_ref,
    cour_ref,
    owner_ref,
    cloud_ref,
    wide,
    slabs,
    odd,
    even,
    outs,
    give,
    take,
    fsend,
    fland,
    coef,
    bulk,
    late,
    heap,
    late_heap,
    mine,
    summed,
    inc,
    pack,
    load_sem,
    out_sem,
    halo_send,
    halo_recv,
    swap_sem,
    sum_sem,
    meet,
):
    fields, levels, cells, columns = x_hbm.shape
    chunks = columns // LANES
    groups, cap = fland.shape[:2]
    peers = lax.axis_size("grp")
    z_me = lax.axis_index("grp")
    c_me = lax.axis_index("col")
    direct = cells % 8 == 0
    reach = 1 if direct else DEPTH // cells
    width = cells + 2 * DEPTH
    own = TOP + DEPTH
    full, edges = level_edges(levels)
    split = split_level(fields, levels, chunks, peers, edges[full] - BLOCK)
    kept = fields * levels * (chunks - 1)
    span = lambda i: pl.ds(i * LANES, LANES)

    loads = []
    for c in range(chunks):
        if direct:
            target = wide.at[c, :, :, own : own + cells, :]
        else:
            target = slabs.at[c, 2 * reach]
        load = pltpu.make_async_copy(x_hbm.at[:, :, :, span(c)], target, load_sem.at[c])
        load.start()
        loads.append(load)
    small = []
    pairs = ((prof_hbm, prof_ref), (cour_hbm, cour_ref), (owner_hbm, owner_ref), (cloud_hbm, cloud_ref))
    for i, (source, target) in enumerate(pairs):
        load = pltpu.make_async_copy(source, target, load_sem.at[chunks + i])
        load.start()
        small.append(load)

    def remote(source, target, send, recv, axis, peer):
        return pltpu.make_async_remote_copy(
            src_ref=source,
            dst_ref=target,
            send_sem=send,
            recv_sem=recv,
            device_id={axis: peer},
            device_id_type=MESH,
        )

    def received(ref, sem):
        remote(ref, ref, sem, sem, "grp", z_me).wait_recv()

    def sent(ref, sem):
        remote(ref, ref, sem, sem, "grp", z_me).wait_send()

    def send_slabs(c, b):
        rows = pl.ds(edges[b], edges[b + 1] - edges[b])
        for j in range(1, reach + 1):
            for side in range(2):
                peer = lax.rem(z_me + (peers - j if side == 0 else j), peers)
                source = slabs.at[c, 2 * reach, :, rows]
                target = slabs.at[c, 2 * (j - 1) + side, :, rows]
                remote(source, target, halo_send.at[0], halo_recv.at[c, b], "grp", peer).start()

    lead = jnp.where(z_me == peers - 1, 1, 0)
    items = [(c, b) for c in range(chunks) for b in range(len(edges) - 1)]

    def send_rows(i, side):
        c, b = items[i]
        rows = pl.ds(edges[b], edges[b + 1] - edges[b])
        peer = lax.rem(z_me + side + (1 - side) * (peers - 1), peers)
        near = pl.multiple_of(own + side * (cells - DEPTH), 8)
        far = pl.multiple_of(own + cells - side * (cells + DEPTH), 8)
        source = wide.at[c, :, rows, pl.ds(near, DEPTH), :]
        target = wide.at[c, :, rows, pl.ds(far, DEPTH), :]
        remote(source, target, halo_send.at[0], halo_recv.at[c, b], "grp", peer).start()

    barrier = pltpu.get_barrier_semaphore()

    def signal(sem, axis, peer):
        pl.semaphore_signal(sem, inc=1, device_id={axis: peer}, device_id_type=MESH)

    if direct and peers > 2 and groups & (groups - 1) == 0:
        at_left, at_right = z_me == 0, z_me == peers - 1
        ends = at_left | at_right
        bits = [1 << i for i in range(groups.bit_length() - 1)]
        across = [flip(c_me, k) for k in bits]

        @pl.when(z_me > 0)
        def _():
            signal(barrier, "grp", z_me - 1)

        @pl.when(z_me < peers - 1)
        def _():
            signal(barrier, "grp", z_me + 1)

        for peer in across:
            signal(barrier, "col", peer)
        with jax.named_scope("barrier"):
            pl.semaphore_wait(barrier, len(bits) + 2 - jnp.where(ends, 1, 0))
        with jax.named_scope("send"):
            loads[0].wait()
            for i in range(AHEAD):
                send_rows(i, 1 - lead)

            @pl.when(jnp.logical_not(ends))
            def _():
                for i in range(AHEAD):
                    send_rows(i, lead)

            @pl.when((z_me > 0) & (z_me < peers - 1))
            def _():
                signal(meet.at[0], "grp", z_me - 1)
                signal(meet.at[1], "grp", z_me + 1)

            for r in range(peers - 2):

                @pl.when(r < peers - 2 - z_me)
                def _():
                    pl.semaphore_wait(meet.at[0], 1)

                    @pl.when(z_me > 0)
                    def _():
                        signal(meet.at[0], "grp", z_me - 1)

                @pl.when(r < z_me - 1)
                def _():
                    pl.semaphore_wait(meet.at[1], 1)

                    @pl.when(z_me < peers - 1)
                    def _():
                        signal(meet.at[1], "grp", z_me + 1)

            @pl.when(ends)
            def _():
                for i in range(AHEAD):
                    send_rows(i, lead)

            for load in loads[1:]:
                load.wait()
            for i in range(AHEAD, AHEAD + LEAD):
                send_rows(i, lead)
            for i in range(AHEAD, len(items)):
                send_rows(i, 1 - lead)
                if i + LEAD < len(items):
                    send_rows(i + LEAD, lead)
            for i, peer in enumerate(across[1:]):
                signal(meet.at[2 + i], "col", peer)
                pl.semaphore_wait(meet.at[2 + i], 1)
    else:
        for k in range(1, peers):
            signal(barrier, "grp", lax.rem(z_me + k, peers))
        for k in range(1, groups):
            signal(barrier, "col", lax.rem(c_me + k, groups))
        pl.semaphore_wait(barrier, peers - 1 + groups - 1)
        for load in loads:
            load.wait()
        for i, (c, b) in enumerate(items):
            if direct:
                send_rows(i, 0)
                send_rows(i, 1)
            else:
                send_slabs(c, b)

    with jax.named_scope("forcing"):
        for load in small:
            load.wait()
        owner = jnp.concatenate(
            [owner_ref[pl.ds(c, groups, stride=chunks), :] for c in range(chunks)], axis=1
        )
        own_row = jnp.concatenate(
            [owner_ref[pl.ds(c_me * chunks + c, 1), :] for c in range(chunks)], axis=1
        )
        group_ids = lax.broadcasted_iota(jnp.int32, (groups, columns), 0)
        earlier = (
            lax.broadcasted_iota(jnp.int32, (columns, columns), 0)
            < lax.broadcasted_iota(jnp.int32, (columns, columns), 1)
        ).astype(jnp.float32)
        slot = lax.broadcasted_iota(jnp.int32, (cap, columns), 0).astype(jnp.float32)
        spot = lax.broadcasted_iota(jnp.int32, (cap, columns), 1).astype(jnp.float32) + 1.0

        def ranked(hits):
            rank = jnp.dot(hits, earlier, preferred_element_type=jnp.float32)
            return jnp.where(hits > 0.5, rank, -1.0)

        low = own_row - group_ids * columns
        order = ranked(jnp.where((low >= 0) & (low < columns), 1.0, 0.0))
        for q in range(groups):
            hot = jnp.where(order[q : q + 1] == slot, 1.0, 0.0)
            give[q * cap : (q + 1) * cap, :] = hot
        give_out = pltpu.make_async_copy(give, give_hbm, out_sem.at[0])
        give_out.start()

        for f, ref in ((0, prof_ref), (1, cour_ref)):
            lines = ref.shape[0]
            fsend[:, :, f * LANES : f * LANES + lines] = pick(
                parts_of(ref[...]), give[...].astype(jnp.bfloat16), ((1,), (1,)), swap=True
            ).reshape(groups, cap, lines)
        for k in range(1, groups):
            peer = lax.rem(c_me + k, groups)
            remote(
                fsend.at[peer], fland.at[c_me], swap_sem.at[0], swap_sem.at[1], "col", peer
            ).start()
        fland[c_me] = fsend[c_me]

        local = owner - c_me * columns
        order = ranked(jnp.where((local >= 0) & (local < columns), 1.0, 0.0))
        place = (local + 1).astype(jnp.float32)
        for q in range(groups):
            chosen = jnp.where(order[q : q + 1] == slot, place[q : q + 1], 0.0)
            chosen = jnp.sum(chosen, axis=1, keepdims=True)
            take[q * cap : (q + 1) * cap, :] = jnp.where(chosen == spot, 1.0, 0.0)
        hot = take[...].astype(jnp.bfloat16)

    with jax.named_scope("force_wait"):
        received(fland.at[pl.ds(0, groups - 1)], swap_sem.at[1])
    with jax.named_scope("force_take"):
        landed = fland[:, :, :LANES].reshape(groups * cap, LANES)
        phys = pick(parts_of(landed), hot, ((0,), (0,))) / STEPS
        landed = fland[:, :, LANES:].reshape(groups * cap, LANES)
        speed = 0.5 * pick(parts_of(landed), hot, ((0,), (0,)))
        for c in range(chunks):
            lanes = slice(c * LANES, (c + 1) * LANES)
            west = diffuse_x + speed[:levels, lanes]
            east = diffuse_x - speed[:levels, lanes]
            heat = SCALE * phys[:levels, lanes]
            rain = phys[levels : 2 * levels, lanes]
            rows = (SCALE * west, west, SCALE * east, east, heat - 1.0, rain + sat_scale, heat, rain)
            for i, row in enumerate(rows):
                coef[c, i] = row
    rain_gain = cond_rate * cloud_ref[...].astype(jnp.float32)
    heat_gain = (latent_gain * SCALE) * rain_gain

    def stepped(c, s, z):
        rows = width - 2 * s if s == STEPS else round_up(width - 2 * s, 8)
        first = TOP + (width - rows) // 2
        source = wide.at[c] if s == 1 else (odd if s % 2 == 0 else even)
        if isinstance(z, int):
            up, down = min(z + 1, levels - 1), max(z - 1, 0)
        else:
            up, down = jnp.minimum(z + 1, levels - 1), jnp.maximum(z - 1, 0)
        lanes = slice(c * LANES, (c + 1) * LANES)
        new = []
        for f in range(fields):
            scale = SCALE if s == 1 and f == 0 else 1.0
            pick_row = lambda i: coef[c, i, pl.ds(z, 1), :]
            west_gain = pick_row(0 if scale != 1.0 else 1)
            east_gain = pick_row(2 if scale != 1.0 else 3)
            push = pick_row((4 if s == 1 else 6) + f)
            here = source[f, z, first : first + rows]
            west = source[f, z, first - 1 : first - 1 + rows]
            east = source[f, z, first + 1 : first + 1 + rows]
            upper = source[f, up, first : first + rows]
            lower = source[f, down, first : first + rows]
            new.append(
                (
                    (scale * (1.0 - 2.0 * diffuse_x - 2.0 * diffuse_z)) * here
                    + (scale * diffuse_z) * (upper + lower)
                )
                + ((west_gain * west + east_gain * east) + push)
            )
        energy, moisture = new
        excess = jnp.maximum(moisture - jnp.exp2(energy), 0.0)
        energy = energy + excess * heat_gain[:, lanes]
        moisture = moisture - excess * rain_gain[:, lanes]
        if s == STEPS:
            energy = energy * (1.0 / SCALE) + 1.0 / SCALE
            moisture = moisture - sat_scale
        return first, rows, (energy, moisture)

    def keep_row(f, z, total):
        def early():
            bulk[pl.ds(kept + f * split + z, 1), :] = total

        def later():
            late[pl.ds(f * (levels - split) + z - split, 1), :] = total

        if isinstance(z, int):
            (early if z < split else later)()
        else:
            pl.when(z < split)(early)
            pl.when(z >= split)(later)

    def put(c, s, z, result):
        first, rows, values = result
        target = odd if s % 2 else even
        for f, value in enumerate(values):
            if s == STEPS:
                outs[f, z, :, c * LANES : (c + 1) * LANES] = value
                if direct:
                    old = wide[c, f, z, own : own + cells]
                else:
                    old = slabs[c, 2 * reach, f, z]
                total = jnp.sum(value - old, axis=0, keepdims=True)
                if c < chunks - 1:
                    bulk[pl.ds((c * fields + f) * levels + z, 1), :] = total
                else:
                    keep_row(f, z, total)
            else:
                target[f, z, first : first + rows] = value

    def sweep(c, s, low, count, unroll):
        def body(i, carry):
            z = low + unroll * i
            results = [stepped(c, s, z + k) for k in range(unroll)]
            for k in range(unroll):
                put(c, s, z + k, results[k])
            return carry

        trips = count // unroll
        if trips == 1:
            body(0, 0)
        elif trips > 1:
            lax.fori_loop(0, trips, body, 0)
        rest = [low + k for k in range(trips * unroll, count)]
        results = [stepped(c, s, z) for z in rest]
        for z, result in zip(rest, results):
            put(c, s, z, result)

    def arrive(c, b, start, count):
        rows = pl.ds(start, count)
        if direct:
            received(wide.at[c, :, rows, TOP : TOP + 2 * DEPTH, :], halo_recv.at[c, b])
        else:
            received(slabs.at[c, pl.ds(0, 2 * reach), :, rows], halo_recv.at[c, b])

            def fill(z, carry):
                for f in range(fields):
                    wide[c, f, z, own : own + cells] = slabs[c, 2 * reach, f, z]
                    for j in range(1, reach + 1):
                        right = own + j * cells
                        left = own - j * cells
                        wide[c, f, z, right : right + cells] = slabs[c, 2 * j - 2, f, z]
                        wide[c, f, z, left : left + cells] = slabs[c, 2 * j - 1, f, z]
                return carry

            lax.fori_loop(start, start + count, fill, 0)

    def opening(c, stop):
        with jax.named_scope(f"first#c={c}"):
            arrive(c, 0, 0, BLOCK)
            for s in range(1, STEPS + 1):
                sweep(c, s, 0, BLOCK - s, 2)

        def body(b, carry):
            with jax.named_scope("arrive"):
                arrive(c, b, b * BLOCK, BLOCK)
            with jax.named_scope("steps"):
                for s in range(1, STEPS + 1):
                    sweep(c, s, b * BLOCK - s, BLOCK, 4)
            return carry

        lax.fori_loop(1, stop, body, 0)

    def scatter(part, landing, sem):
        lines = part.shape[0] // peers
        for k in range(1, peers):
            peer = lax.rem(z_me + k, peers)
            block = pl.ds(pl.multiple_of(peer * lines, lines), lines)
            remote(part.at[block], landing.at[k - 1], sem.at[0], sem.at[1], "grp", peer).start()

    def gather(part, landing, piece, result, sem, sem2):
        lines = part.shape[0] // peers
        block = pl.ds(pl.multiple_of(z_me * lines, lines), lines)
        total = part[block, :]
        received(landing, sem.at[1])
        for k in range(peers - 1):
            total = total + landing[k]
        piece[...] = total
        result[block, :] = total
        for k in range(1, peers):
            peer = lax.rem(z_me + k, peers)
            remote(piece, result.at[block], sem2.at[0], sem2.at[1], "grp", peer).start()

    def others(ref):
        return ref.at[pl.ds(0, ref.shape[0] // peers * (peers - 1))]

    last = chunks - 1
    if bulk.shape[0] > kept + fields * split:
        bulk[kept + fields * split :, :] = jnp.zeros_like(bulk[kept + fields * split :, :])
    if late.shape[0] > fields * (levels - split):
        late[fields * (levels - split) :, :] = jnp.zeros_like(late[fields * (levels - split) :, :])
    for c in range(last):
        opening(c, full)
        for b in range(full, len(edges) - 1):
            arrive(c, b, edges[b], edges[b + 1] - edges[b])
        with jax.named_scope("closing"):
            for s in range(1, STEPS + 1):
                sweep(c, s, edges[full] - s, levels - edges[full] + s, 2)
        pltpu.make_async_copy(
            outs.at[:, :, :, span(c)], final_hbm.at[:, :, :, span(c)], out_sem.at[1]
        ).start()
    ready = edges[full] - BLOCK
    opening(last, full)
    for b in range(full, len(edges) - 1):
        if b == full:
            scatter(bulk, heap, sum_sem.at[0])
            pltpu.make_async_copy(
                outs.at[:, pl.ds(0, ready), :, span(last)],
                final_hbm.at[:, pl.ds(0, ready), :, span(last)],
                out_sem.at[1],
            ).start()
        with jax.named_scope(f"late_arrive#b={b}"):
            arrive(last, b, edges[b], edges[b + 1] - edges[b])
        with jax.named_scope(f"late_steps#b={b}"):
            ends = b == len(edges) - 2
            for s in range(1, STEPS + 1):
                count = edges[b + 1] - edges[b] + (s if ends else 0)
                sweep(last, s, edges[b] - s, count, count if ends else 4)
    late_sem = sum_sem.at[2]
    for k in range(peers - 1, 0, -1):
        remote(late, late_heap.at[k - 1], late_sem.at[0], late_sem.at[1], "grp", flip(z_me, k)).start()
    pltpu.make_async_copy(
        outs.at[:, pl.ds(ready, levels - ready), :, span(last)],
        final_hbm.at[:, pl.ds(ready, levels - ready), :, span(last)],
        out_sem.at[1],
    ).start()
    with jax.named_scope("scatter_wait"):
        gather(bulk, heap, mine, summed, sum_sem.at[0], sum_sem.at[1])
    with jax.named_scope("late_wait"):
        received(late_heap, late_sem.at[1])
        totals = [late[...]] + [late_heap[k] for k in range(peers - 1)]
        while len(totals) > 1:
            totals = [x + y for x, y in zip(totals[::2], totals[1::2])]
        for f in range(fields):
            inc[last, f * levels + split : (f + 1) * levels, :] = totals[0][
                f * (levels - split) : (f + 1) * (levels - split)
            ]
        inc[last, fields * levels :, :] = jnp.zeros_like(inc[last, fields * levels :, :])
        for c in range(last):
            inc[c, fields * levels :, :] = jnp.zeros_like(inc[c, fields * levels :, :])
    with jax.named_scope("gather_wait"):
        received(others(summed), sum_sem.at[1, 1])
    with jax.named_scope("pack"):
        for c in range(last):
            start = c * fields * levels
            inc[c, : fields * levels, :] = summed[start : start + fields * levels, :]
        for f in range(fields):
            start = kept + f * split
            inc[last, f * levels : f * levels + split, :] = summed[start : start + split, :]
        packed = 0.0
        for c in range(chunks):
            packed = packed + pick(
                parts_of(inc[c]), hot[:, c * LANES : (c + 1) * LANES], ((1,), (1,)), swap=True
            )
        pack[...] = (packed / (cells * peers)).reshape(pack.shape)
    for k in sorted(range(1, groups), key=lambda k: -bin(k >> 1).count("1")):
        peer = flip(c_me, k)
        remote(pack.at[peer], land.at[c_me], swap_sem.at[2], swap_sem.at[3], "col", peer).start()
    keep = pltpu.make_async_copy(pack.at[c_me], land.at[c_me], out_sem.at[2])
    keep.start()
    with jax.named_scope("drain"):
        if direct:
            sent(wide.at[:, :, :, TOP : TOP + 2 * DEPTH, :], halo_send.at[0])
        else:
            sent(slabs.at[:, pl.ds(0, 2 * reach)], halo_send.at[0])
        sent(fsend.at[pl.ds(0, groups - 1)], swap_sem.at[0])
        sent(others(summed), sum_sem.at[0, 0])
        sent(others(summed), sum_sem.at[1, 0])
        sent(late_heap, late_sem.at[0])
        give_out.wait()
        pltpu.make_async_copy(outs, final_hbm, out_sem.at[1]).wait()
        keep.wait()
        sent(pack.at[pl.ds(0, groups - 1)], swap_sem.at[2])
    with jax.named_scope("return_wait"):
        received(land.at[pl.ds(0, groups - 1)], swap_sem.at[3])


def finish_kernel(
    land_hbm, give_hbm, state_hbm, tend_hbm, final_hbm, land, give, state, tend, in_sem, out_sem
):
    fields, levels = state.shape[:2]
    groups, cap, rows = land.shape
    small = [
        pltpu.make_async_copy(land_hbm, land, in_sem.at[0]),
        pltpu.make_async_copy(give_hbm, give, in_sem.at[1]),
    ]
    cuts = [levels * i // PIECES for i in range(PIECES + 1)]
    pieces = [(f, pl.ds(a, b - a)) for f in range(fields) for a, b in zip(cuts, cuts[1:])]
    ins = [
        pltpu.make_async_copy(state_hbm.at[f, z], state.at[f, z], in_sem.at[2 + i])
        for i, (f, z) in enumerate(pieces)
    ]
    stores = [
        pltpu.make_async_copy(state.at[f, z], final_hbm.at[f, z], out_sem.at[i])
        for i, (f, z) in enumerate(pieces)
    ]
    for copy in small + ins:
        copy.start()
    for copy in small:
        copy.wait()
    split = parts_of(land[...].reshape(groups * cap, rows))
    hot = give[...].astype(jnp.bfloat16)
    for load, store in zip(ins, stores):
        load.wait()
        store.start()
    back = pick(split, hot, ((0,), (0,)))
    tend[...] = back[: tend.shape[0]]
    store = pltpu.make_async_copy(tend, tend_hbm, out_sem.at[len(pieces)])
    store.start()
    for copy in stores + [store]:
        copy.wait()


def on_device(profiles, courant, owner_map, cloud_flags, crm_state):
    columns = profiles.shape[0]
    fields, levels, cells = crm_state.shape[:3]
    groups = lax.axis_size("col")
    peers = lax.axis_size("grp")
    per_peer = columns // groups
    cap = round_up(per_peer + min(2, per_peer), 8)
    chunks = columns // LANES
    direct = cells % 8 == 0
    reach = 1 if direct else DEPTH // cells
    full, edges = level_edges(levels)
    split = split_level(fields, levels, chunks, peers, edges[full] - BLOCK)
    rows = round_up(fields * levels, LANES)
    bulk_rows = round_up(fields * (levels * (chunks - 1) + split), 8 * peers)
    late_rows = round_up(fields * (levels - split), 8)
    f32 = lambda *shape: pltpu.VMEM(shape, jnp.float32)
    i32 = lambda *shape: pltpu.VMEM(shape, jnp.int32)
    dma = lambda *shape: pltpu.SemaphoreType.DMA(shape)
    anywhere = pl.BlockSpec(memory_space=pl.ANY)
    tall = round_up(TOP + cells + 2 * DEPTH + 1, 8)
    slabs = (8, 128) if direct else (chunks, 2 * reach + 1, fields, levels, cells, LANES)
    land, give, state = pl.pallas_call(
        window_kernel,
        out_shape=(
            jax.ShapeDtypeStruct((groups, cap, rows), jnp.float32),
            jax.ShapeDtypeStruct((groups * cap, columns), jnp.float32),
            jax.ShapeDtypeStruct(crm_state.shape, jnp.float32),
        ),
        in_specs=[anywhere] * 5,
        out_specs=(anywhere,) * 3,
        scratch_shapes=[
            f32(fields * levels, columns),
            f32(levels, columns),
            i32(groups * chunks, LANES),
            i32(1, columns),
            f32(chunks, fields, levels, tall, LANES),
            f32(*slabs),
            f32(fields, levels, tall, LANES),
            f32(fields, levels, tall, LANES),
            f32(fields, levels, cells, columns),
            f32(groups * cap, columns),
            f32(groups * cap, columns),
            f32(groups, cap, 2 * LANES),
            f32(groups, cap, 2 * LANES),
            f32(chunks, 8, levels, LANES),
            f32(bulk_rows, LANES),
            f32(late_rows, LANES),
            f32(peers - 1, bulk_rows // peers, LANES),
            f32(peers - 1, late_rows, LANES),
            f32(bulk_rows // peers, LANES),
            f32(bulk_rows, LANES),
            f32(chunks, rows, LANES),
            f32(groups, cap, rows),
            dma(chunks + 4),
            dma(3),
            dma(1),
            dma(chunks, len(edges) - 1),
            dma(4),
            dma(3, 2),
            pltpu.SemaphoreType.REGULAR((max(2, groups.bit_length()),)),
        ],
        compiler_params=pltpu.CompilerParams(
            collective_id=0, has_side_effects=True, vmem_limit_bytes=LIMIT
        ),
    )(
        profiles.T,
        courant.T,
        owner_map.reshape(groups * chunks, LANES),
        cloud_flags[None, :],
        crm_state,
    )
    tendency, final = pl.pallas_call(
        finish_kernel,
        out_shape=(
            jax.ShapeDtypeStruct((fields * levels, columns), jnp.float32),
            jax.ShapeDtypeStruct(crm_state.shape, jnp.float32),
        ),
        in_specs=[anywhere] * 3,
        out_specs=(anywhere,) * 2,
        scratch_shapes=[
            f32(groups, cap, rows),
            f32(groups * cap, columns),
            f32(*crm_state.shape),
            f32(fields * levels, columns),
            dma(2 + PIECES * fields),
            dma(1 + PIECES * fields),
        ],
        compiler_params=pltpu.CompilerParams(vmem_limit_bytes=LIMIT),
    )(land, give, state)
    return tendency.T, final


def solution(mesh):
    placed = (P("col", None), P("col", None), P(), P("col"), P(None, None, "grp", "col"))
    return jax.shard_map(
        on_device,
        mesh=mesh,
        in_specs=placed,
        out_specs=(P("col", None), P(None, None, "grp", "col")),
        check_vma=False,
    )
```

```python
import jax
import jax.numpy as jnp
from jax import lax
from jax.experimental import pallas as pl
from jax.experimental.pallas import tpu as pltpu
from jax.sharding import PartitionSpec as P

STEPS = 8
DEPTH = STEPS
BLOCK = 8
PIECE = 4
AHEAD = 2
LEAD = 1
PIECES = 2
LANES = 128
LIMIT = 67_043_328
TOP = 8
MESH = pl.DeviceIdType.MESH

diffuse_x = 0.25
diffuse_z = 0.2
sat_scale = 0.5
sat_slope = 0.3
cond_rate = 0.5
latent_gain = 0.4
SCALE = sat_slope * 1.4426950408889634


def round_up(n, m):
    return -(-n // m) * m


def parts_of(x):
    high = x.astype(jnp.bfloat16)
    rest = x - high.astype(jnp.float32)
    middle = rest.astype(jnp.bfloat16)
    return high, middle, (rest - middle.astype(jnp.float32)).astype(jnp.bfloat16)


def pick(parts, hot, dims, swap=False):
    total = 0.0
    for part in parts:
        pair = (hot, part) if swap else (part, hot)
        total = total + lax.dot_general(
            *pair, (dims, ((), ())), preferred_element_type=jnp.float32
        )
    return total


def split_level(fields, levels, chunks, peers, limit):
    for split in range(limit, 0, -1):
        if fields * (levels * (chunks - 1) + split) % (8 * peers) == 0:
            return split
    return limit


def flip(index, mask):
    place = index
    for i in range(mask.bit_length()):
        if mask >> i & 1:
            place = place + (1 << i) - (2 << i) * lax.rem(lax.div(index, 1 << i), 2)
    return place


def level_edges(levels):
    full = max(2, (levels - BLOCK) // BLOCK)
    edges = [i * BLOCK for i in range(full + 1)]
    while edges[-1] < levels:
        edges.append(min(edges[-1] + PIECE, levels))
    return full, edges


def window_kernel(
    prof_hbm,
    cour_hbm,
    owner_hbm,
    cloud_hbm,
    x_hbm,
    land,
    give_hbm,
    final_hbm,
    prof_ref,
    cour_ref,
    owner_ref,
    cloud_ref,
    wide,
    slabs,
    odd,
    even,
    outs,
    give,
    take,
    fsend,
    fland,
    coef,
    bulk,
    late,
    heap,
    late_heap,
    mine,
    summed,
    inc,
    pack,
    load_sem,
    out_sem,
    halo_send,
    halo_recv,
    swap_sem,
    sum_sem,
    meet,
):
    fields, levels, cells, columns = x_hbm.shape
    chunks = columns // LANES
    groups, cap = fland.shape[:2]
    peers = lax.axis_size("grp")
    z_me = lax.axis_index("grp")
    c_me = lax.axis_index("col")
    direct = cells % 8 == 0
    reach = 1 if direct else DEPTH // cells
    width = cells + 2 * DEPTH
    own = TOP + DEPTH
    full, edges = level_edges(levels)
    split = split_level(fields, levels, chunks, peers, edges[full] - BLOCK)
    kept = fields * levels * (chunks - 1)
    span = lambda i: pl.ds(i * LANES, LANES)

    loads = []
    for c in range(chunks):
        if direct:
            target = wide.at[c, :, :, own : own + cells, :]
        else:
            target = slabs.at[c, 2 * reach]
        load = pltpu.make_async_copy(x_hbm.at[:, :, :, span(c)], target, load_sem.at[c])
        load.start()
        loads.append(load)
    small = []
    pairs = ((prof_hbm, prof_ref), (cour_hbm, cour_ref), (owner_hbm, owner_ref), (cloud_hbm, cloud_ref))
    for i, (source, target) in enumerate(pairs):
        load = pltpu.make_async_copy(source, target, load_sem.at[chunks + i])
        load.start()
        small.append(load)

    def remote(source, target, send, recv, axis, peer):
        return pltpu.make_async_remote_copy(
            src_ref=source,
            dst_ref=target,
            send_sem=send,
            recv_sem=recv,
            device_id={axis: peer},
            device_id_type=MESH,
        )

    def received(ref, sem):
        remote(ref, ref, sem, sem, "grp", z_me).wait_recv()

    def sent(ref, sem):
        remote(ref, ref, sem, sem, "grp", z_me).wait_send()

    def send_slabs(c, b):
        rows = pl.ds(edges[b], stop(c, b) - edges[b])
        for j in range(1, reach + 1):
            for side in range(2):
                peer = lax.rem(z_me + (peers - j if side == 0 else j), peers)
                source = slabs.at[c, 2 * reach, :, rows]
                target = slabs.at[c, 2 * (j - 1) + side, :, rows]
                remote(source, target, halo_send.at[0], landed_at(c, b), "grp", peer).start()

    lead = jnp.where(z_me == peers - 1, 1, 0)
    items = [
        (c, b) for c in range(chunks) for b in range(full + 1 if c < chunks - 1 else len(edges) - 1)
    ]
    stop = lambda c, b: levels if c < chunks - 1 and b == full else edges[b + 1]
    landed_at = lambda c, b: halo_recv.at[c * (full + 1) + b]

    def send_rows(i, side):
        c, b = items[i]
        rows = pl.ds(edges[b], stop(c, b) - edges[b])
        peer = lax.rem(z_me + side + (1 - side) * (peers - 1), peers)
        near = pl.multiple_of(own + side * (cells - DEPTH), 8)
        far = pl.multiple_of(own + cells - side * (cells + DEPTH), 8)
        source = wide.at[c, :, rows, pl.ds(near, DEPTH), :]
        target = wide.at[c, :, rows, pl.ds(far, DEPTH), :]
        remote(source, target, halo_send.at[0], landed_at(c, b), "grp", peer).start()

    barrier = pltpu.get_barrier_semaphore()

    def signal(sem, axis, peer):
        pl.semaphore_signal(sem, inc=1, device_id={axis: peer}, device_id_type=MESH)

    if direct and peers > 2 and groups & (groups - 1) == 0:
        at_left, at_right = z_me == 0, z_me == peers - 1
        ends = at_left | at_right
        bits = [1 << i for i in range(groups.bit_length() - 1)]
        across = [flip(c_me, k) for k in bits]

        @pl.when(z_me > 0)
        def _():
            signal(barrier, "grp", z_me - 1)

        @pl.when(z_me < peers - 1)
        def _():
            signal(barrier, "grp", z_me + 1)

        for peer in across:
            signal(barrier, "col", peer)
        with jax.named_scope("barrier"):
            pl.semaphore_wait(barrier, len(bits) + 2 - jnp.where(ends, 1, 0))
        with jax.named_scope("send"):
            loads[0].wait()
            for i in range(AHEAD):
                send_rows(i, 1 - lead)

            @pl.when(jnp.logical_not(ends))
            def _():
                for i in range(AHEAD):
                    send_rows(i, lead)

            @pl.when((z_me > 0) & (z_me < peers - 1))
            def _():
                signal(meet.at[0], "grp", z_me - 1)
                signal(meet.at[1], "grp", z_me + 1)

            for r in range(peers - 2):

                @pl.when(r < peers - 2 - z_me)
                def _():
                    pl.semaphore_wait(meet.at[0], 1)

                    @pl.when(z_me > 0)
                    def _():
                        signal(meet.at[0], "grp", z_me - 1)

                @pl.when(r < z_me - 1)
                def _():
                    pl.semaphore_wait(meet.at[1], 1)

                    @pl.when(z_me < peers - 1)
                    def _():
                        signal(meet.at[1], "grp", z_me + 1)

            @pl.when(ends)
            def _():
                for i in range(AHEAD):
                    send_rows(i, lead)

            for load in loads[1:]:
                load.wait()
            for i in range(AHEAD, AHEAD + LEAD):
                send_rows(i, lead)
            for i in range(AHEAD, len(items)):
                send_rows(i, 1 - lead)
                if i + LEAD < len(items):
                    send_rows(i + LEAD, lead)
            for i, peer in enumerate(across[1:]):
                signal(meet.at[2 + i], "col", peer)
                pl.semaphore_wait(meet.at[2 + i], 1)
    else:
        for k in range(1, peers):
            signal(barrier, "grp", lax.rem(z_me + k, peers))
        for k in range(1, groups):
            signal(barrier, "col", lax.rem(c_me + k, groups))
        pl.semaphore_wait(barrier, peers - 1 + groups - 1)
        for load in loads:
            load.wait()
        for i, (c, b) in enumerate(items):
            if direct:
                send_rows(i, 0)
                send_rows(i, 1)
            else:
                send_slabs(c, b)

    with jax.named_scope("forcing"):
        for load in small:
            load.wait()
        owner = jnp.concatenate(
            [owner_ref[pl.ds(c, groups, stride=chunks), :] for c in range(chunks)], axis=1
        )
        own_row = jnp.concatenate(
            [owner_ref[pl.ds(c_me * chunks + c, 1), :] for c in range(chunks)], axis=1
        )
        group_ids = lax.broadcasted_iota(jnp.int32, (groups, columns), 0)
        earlier = (
            lax.broadcasted_iota(jnp.int32, (columns, columns), 0)
            < lax.broadcasted_iota(jnp.int32, (columns, columns), 1)
        ).astype(jnp.float32)
        slot = lax.broadcasted_iota(jnp.int32, (cap, columns), 0).astype(jnp.float32)
        spot = lax.broadcasted_iota(jnp.int32, (cap, columns), 1).astype(jnp.float32) + 1.0

        def ranked(hits):
            rank = jnp.dot(hits, earlier, preferred_element_type=jnp.float32)
            return jnp.where(hits > 0.5, rank, -1.0)

        low = own_row - group_ids * columns
        order = ranked(jnp.where((low >= 0) & (low < columns), 1.0, 0.0))
        for q in range(groups):
            hot = jnp.where(order[q : q + 1] == slot, 1.0, 0.0)
            give[q * cap : (q + 1) * cap, :] = hot
        give_out = pltpu.make_async_copy(give, give_hbm, out_sem.at[0])
        give_out.start()

        for f, ref in ((0, prof_ref), (1, cour_ref)):
            lines = ref.shape[0]
            fsend[:, :, f * LANES : f * LANES + lines] = pick(
                parts_of(ref[...]), give[...].astype(jnp.bfloat16), ((1,), (1,)), swap=True
            ).reshape(groups, cap, lines)
        for k in range(1, groups):
            peer = lax.rem(c_me + k, groups)
            remote(
                fsend.at[peer], fland.at[c_me], swap_sem.at[0], swap_sem.at[1], "col", peer
            ).start()
        fland[c_me] = fsend[c_me]

        local = owner - c_me * columns
        order = ranked(jnp.where((local >= 0) & (local < columns), 1.0, 0.0))
        place = (local + 1).astype(jnp.float32)
        for q in range(groups):
            chosen = jnp.where(order[q : q + 1] == slot, place[q : q + 1], 0.0)
            chosen = jnp.sum(chosen, axis=1, keepdims=True)
            take[q * cap : (q + 1) * cap, :] = jnp.where(chosen == spot, 1.0, 0.0)
        hot = take[...].astype(jnp.bfloat16)

    with jax.named_scope("force_wait"):
        received(fland.at[pl.ds(0, groups - 1)], swap_sem.at[1])
    with jax.named_scope("force_take"):
        landed = fland[:, :, :LANES].reshape(groups * cap, LANES)
        phys = pick(parts_of(landed), hot, ((0,), (0,))) / STEPS
        landed = fland[:, :, LANES:].reshape(groups * cap, LANES)
        speed = 0.5 * pick(parts_of(landed), hot, ((0,), (0,)))
        for c in range(chunks):
            lanes = slice(c * LANES, (c + 1) * LANES)
            west = diffuse_x + speed[:levels, lanes]
            east = diffuse_x - speed[:levels, lanes]
            heat = SCALE * phys[:levels, lanes]
            rain = phys[levels : 2 * levels, lanes]
            rows = (SCALE * west, west, SCALE * east, east, heat - 1.0, rain + sat_scale, heat, rain)
            for i, row in enumerate(rows):
                coef[c, i] = row
    rain_gain = cond_rate * cloud_ref[...].astype(jnp.float32)
    heat_gain = (latent_gain * SCALE) * rain_gain

    def stepped(c, s, z):
        rows = width - 2 * s if s == STEPS else round_up(width - 2 * s, 8)
        first = TOP + (width - rows) // 2
        source = wide.at[c] if s == 1 else (odd if s % 2 == 0 else even)
        if isinstance(z, int):
            up, down = min(z + 1, levels - 1), max(z - 1, 0)
        else:
            up, down = jnp.minimum(z + 1, levels - 1), jnp.maximum(z - 1, 0)
        lanes = slice(c * LANES, (c + 1) * LANES)
        new = []
        for f in range(fields):
            scale = SCALE if s == 1 and f == 0 else 1.0
            pick_row = lambda i: coef[c, i, pl.ds(z, 1), :]
            west_gain = pick_row(0 if scale != 1.0 else 1)
            east_gain = pick_row(2 if scale != 1.0 else 3)
            push = pick_row((4 if s == 1 else 6) + f)
            here = source[f, z, first : first + rows]
            west = source[f, z, first - 1 : first - 1 + rows]
            east = source[f, z, first + 1 : first + 1 + rows]
            upper = source[f, up, first : first + rows]
            lower = source[f, down, first : first + rows]
            new.append(
                (
                    (scale * (1.0 - 2.0 * diffuse_x - 2.0 * diffuse_z)) * here
                    + (scale * diffuse_z) * (upper + lower)
                )
                + ((west_gain * west + east_gain * east) + push)
            )
        energy, moisture = new
        excess = jnp.maximum(moisture - jnp.exp2(energy), 0.0)
        energy = energy + excess * heat_gain[:, lanes]
        moisture = moisture - excess * rain_gain[:, lanes]
        if s == STEPS:
            energy = energy * (1.0 / SCALE) + 1.0 / SCALE
            moisture = moisture - sat_scale
        return first, rows, (energy, moisture)

    def keep_row(f, z, total):
        def early():
            bulk[pl.ds(kept + f * split + z, 1), :] = total

        def later():
            late[pl.ds(f * (levels - split) + z - split, 1), :] = total

        if isinstance(z, int):
            (early if z < split else later)()
        else:
            pl.when(z < split)(early)
            pl.when(z >= split)(later)

    def put(c, s, z, result):
        first, rows, values = result
        target = odd if s % 2 else even
        for f, value in enumerate(values):
            if s == STEPS:
                outs[f, z, :, c * LANES : (c + 1) * LANES] = value
                if direct:
                    old = wide[c, f, z, own : own + cells]
                else:
                    old = slabs[c, 2 * reach, f, z]
                total = jnp.sum(value - old, axis=0, keepdims=True)
                if c < chunks - 1:
                    bulk[pl.ds((c * fields + f) * levels + z, 1), :] = total
                else:
                    keep_row(f, z, total)
            else:
                target[f, z, first : first + rows] = value

    def sweep(c, s, low, count, unroll):
        def body(i, carry):
            z = low + unroll * i
            results = [stepped(c, s, z + k) for k in range(unroll)]
            for k in range(unroll):
                put(c, s, z + k, results[k])
            return carry

        trips = count // unroll
        if trips == 1:
            body(0, 0)
        elif trips > 1:
            lax.fori_loop(0, trips, body, 0)
        rest = [low + k for k in range(trips * unroll, count)]
        results = [stepped(c, s, z) for z in rest]
        for z, result in zip(rest, results):
            put(c, s, z, result)

    def arrive(c, b, start, count):
        rows = pl.ds(start, count)
        if direct:
            received(wide.at[c, :, rows, TOP : TOP + 2 * DEPTH, :], landed_at(c, b))
        else:
            received(slabs.at[c, pl.ds(0, 2 * reach), :, rows], landed_at(c, b))

            def fill(z, carry):
                for f in range(fields):
                    wide[c, f, z, own : own + cells] = slabs[c, 2 * reach, f, z]
                    for j in range(1, reach + 1):
                        right = own + j * cells
                        left = own - j * cells
                        wide[c, f, z, right : right + cells] = slabs[c, 2 * j - 2, f, z]
                        wide[c, f, z, left : left + cells] = slabs[c, 2 * j - 1, f, z]
                return carry

            lax.fori_loop(start, start + count, fill, 0)

    def opening(c, stop):
        with jax.named_scope(f"first#c={c}"):
            arrive(c, 0, 0, BLOCK)
            for s in range(1, STEPS + 1):
                sweep(c, s, 0, BLOCK - s, 2)

        def body(b, carry):
            with jax.named_scope("arrive"):
                arrive(c, b, b * BLOCK, BLOCK)
            with jax.named_scope("steps"):
                for s in range(1, STEPS + 1):
                    sweep(c, s, b * BLOCK - s, BLOCK, 4)
            return carry

        lax.fori_loop(1, stop, body, 0)

    def scatter(part, landing, sem):
        lines = part.shape[0] // peers
        for k in range(1, peers):
            peer = lax.rem(z_me + k, peers)
            block = pl.ds(pl.multiple_of(peer * lines, lines), lines)
            remote(part.at[block], landing.at[k - 1], sem.at[0], sem.at[1], "grp", peer).start()

    def gather(part, landing, piece, result, sem, sem2):
        lines = part.shape[0] // peers
        block = pl.ds(pl.multiple_of(z_me * lines, lines), lines)
        total = part[block, :]
        received(landing, sem.at[1])
        for k in range(peers - 1):
            total = total + landing[k]
        piece[...] = total
        result[block, :] = total
        for k in range(1, peers):
            peer = lax.rem(z_me + k, peers)
            remote(piece, result.at[block], sem2.at[0], sem2.at[1], "grp", peer).start()

    def others(ref):
        return ref.at[pl.ds(0, ref.shape[0] // peers * (peers - 1))]

    last = chunks - 1
    if bulk.shape[0] > kept + fields * split:
        bulk[kept + fields * split :, :] = jnp.zeros_like(bulk[kept + fields * split :, :])
    if late.shape[0] > fields * (levels - split):
        late[fields * (levels - split) :, :] = jnp.zeros_like(late[fields * (levels - split) :, :])
    for c in range(last):
        opening(c, full)
        arrive(c, full, edges[full], levels - edges[full])
        with jax.named_scope("closing"):
            for s in range(1, STEPS + 1):
                sweep(c, s, edges[full] - s, levels - edges[full] + s, 2)
        pltpu.make_async_copy(
            outs.at[:, :, :, span(c)], final_hbm.at[:, :, :, span(c)], out_sem.at[1]
        ).start()
    ready = edges[full] - BLOCK
    opening(last, full)
    for b in range(full, len(edges) - 1):
        if b == full:
            scatter(bulk, heap, sum_sem.at[0])
            pltpu.make_async_copy(
                outs.at[:, pl.ds(0, ready), :, span(last)],
                final_hbm.at[:, pl.ds(0, ready), :, span(last)],
                out_sem.at[1],
            ).start()
        with jax.named_scope(f"late_arrive#b={b}"):
            arrive(last, b, edges[b], edges[b + 1] - edges[b])
        with jax.named_scope(f"late_steps#b={b}"):
            ends = b == len(edges) - 2
            for s in range(1, STEPS + 1):
                count = edges[b + 1] - edges[b] + (s if ends else 0)
                sweep(last, s, edges[b] - s, count, count if ends else 4)
    late_sem = sum_sem.at[2]
    for k in range(peers - 1, 0, -1):
        remote(late, late_heap.at[k - 1], late_sem.at[0], late_sem.at[1], "grp", flip(z_me, k)).start()
    pltpu.make_async_copy(
        outs.at[:, pl.ds(ready, levels - ready), :, span(last)],
        final_hbm.at[:, pl.ds(ready, levels - ready), :, span(last)],
        out_sem.at[1],
    ).start()
    with jax.named_scope("scatter_wait"):
        gather(bulk, heap, mine, summed, sum_sem.at[0], sum_sem.at[1])
    with jax.named_scope("late_wait"):
        received(late_heap, late_sem.at[1])
        totals = [late[...]] + [late_heap[k] for k in range(peers - 1)]
        while len(totals) > 1:
            totals = [x + y for x, y in zip(totals[::2], totals[1::2])]
        for f in range(fields):
            inc[last, f * levels + split : (f + 1) * levels, :] = totals[0][
                f * (levels - split) : (f + 1) * (levels - split)
            ]
        inc[last, fields * levels :, :] = jnp.zeros_like(inc[last, fields * levels :, :])
        for c in range(last):
            inc[c, fields * levels :, :] = jnp.zeros_like(inc[c, fields * levels :, :])
    with jax.named_scope("gather_wait"):
        received(others(summed), sum_sem.at[1, 1])
    with jax.named_scope("pack"):
        for c in range(last):
            start = c * fields * levels
            inc[c, : fields * levels, :] = summed[start : start + fields * levels, :]
        for f in range(fields):
            start = kept + f * split
            inc[last, f * levels : f * levels + split, :] = summed[start : start + split, :]
        packed = 0.0
        for c in range(chunks):
            packed = packed + pick(
                parts_of(inc[c]), hot[:, c * LANES : (c + 1) * LANES], ((1,), (1,)), swap=True
            )
        pack[...] = (packed / (cells * peers)).reshape(pack.shape)
    for k in sorted(range(1, groups), key=lambda k: -bin(k >> 1).count("1")):
        peer = flip(c_me, k)
        remote(pack.at[peer], land.at[c_me], swap_sem.at[2], swap_sem.at[3], "col", peer).start()
    keep = pltpu.make_async_copy(pack.at[c_me], land.at[c_me], out_sem.at[2])
    keep.start()
    with jax.named_scope("drain"):
        if direct:
            sent(wide.at[:, :, :, TOP : TOP + 2 * DEPTH, :], halo_send.at[0])
        else:
            sent(slabs.at[:, pl.ds(0, 2 * reach)], halo_send.at[0])
        sent(fsend.at[pl.ds(0, groups - 1)], swap_sem.at[0])
        sent(others(summed), sum_sem.at[0, 0])
        sent(others(summed), sum_sem.at[1, 0])
        sent(late_heap, late_sem.at[0])
        give_out.wait()
        pltpu.make_async_copy(outs, final_hbm, out_sem.at[1]).wait()
        keep.wait()
        sent(pack.at[pl.ds(0, groups - 1)], swap_sem.at[2])
    with jax.named_scope("return_wait"):
        received(land.at[pl.ds(0, groups - 1)], swap_sem.at[3])


def finish_kernel(
    land_hbm, give_hbm, state_hbm, tend_hbm, final_hbm, land, give, state, tend, in_sem, out_sem
):
    fields, levels = state.shape[:2]
    groups, cap, rows = land.shape
    small = [
        pltpu.make_async_copy(land_hbm, land, in_sem.at[0]),
        pltpu.make_async_copy(give_hbm, give, in_sem.at[1]),
    ]
    cuts = [levels * i // PIECES for i in range(PIECES + 1)]
    pieces = [(f, pl.ds(a, b - a)) for f in range(fields) for a, b in zip(cuts, cuts[1:])]
    ins = [
        pltpu.make_async_copy(state_hbm.at[f, z], state.at[f, z], in_sem.at[2 + i])
        for i, (f, z) in enumerate(pieces)
    ]
    stores = [
        pltpu.make_async_copy(state.at[f, z], final_hbm.at[f, z], out_sem.at[i])
        for i, (f, z) in enumerate(pieces)
    ]
    for copy in small + ins:
        copy.start()
    for copy in small:
        copy.wait()
    split = parts_of(land[...].reshape(groups * cap, rows))
    hot = give[...].astype(jnp.bfloat16)
    for load, store in zip(ins, stores):
        load.wait()
        store.start()
    back = pick(split, hot, ((0,), (0,)))
    tend[...] = back[: tend.shape[0]]
    store = pltpu.make_async_copy(tend, tend_hbm, out_sem.at[len(pieces)])
    store.start()
    for copy in stores + [store]:
        copy.wait()


def on_device(profiles, courant, owner_map, cloud_flags, crm_state):
    columns = profiles.shape[0]
    fields, levels, cells = crm_state.shape[:3]
    groups = lax.axis_size("col")
    peers = lax.axis_size("grp")
    per_peer = columns // groups
    cap = round_up(per_peer + min(2, per_peer), 8)
    chunks = columns // LANES
    direct = cells % 8 == 0
    reach = 1 if direct else DEPTH // cells
    full, edges = level_edges(levels)
    split = split_level(fields, levels, chunks, peers, edges[full] - BLOCK)
    rows = round_up(fields * levels, LANES)
    bulk_rows = round_up(fields * (levels * (chunks - 1) + split), 8 * peers)
    late_rows = round_up(fields * (levels - split), 8)
    f32 = lambda *shape: pltpu.VMEM(shape, jnp.float32)
    i32 = lambda *shape: pltpu.VMEM(shape, jnp.int32)
    dma = lambda *shape: pltpu.SemaphoreType.DMA(shape)
    anywhere = pl.BlockSpec(memory_space=pl.ANY)
    tall = round_up(TOP + cells + 2 * DEPTH + 1, 8)
    slabs = (8, 128) if direct else (chunks, 2 * reach + 1, fields, levels, cells, LANES)
    land, give, state = pl.pallas_call(
        window_kernel,
        out_shape=(
            jax.ShapeDtypeStruct((groups, cap, rows), jnp.float32),
            jax.ShapeDtypeStruct((groups * cap, columns), jnp.float32),
            jax.ShapeDtypeStruct(crm_state.shape, jnp.float32),
        ),
        in_specs=[anywhere] * 5,
        out_specs=(anywhere,) * 3,
        scratch_shapes=[
            f32(fields * levels, columns),
            f32(levels, columns),
            i32(groups * chunks, LANES),
            i32(1, columns),
            f32(chunks, fields, levels, tall, LANES),
            f32(*slabs),
            f32(fields, levels, tall, LANES),
            f32(fields, levels, tall, LANES),
            f32(fields, levels, cells, columns),
            f32(groups * cap, columns),
            f32(groups * cap, columns),
            f32(groups, cap, 2 * LANES),
            f32(groups, cap, 2 * LANES),
            f32(chunks, 8, levels, LANES),
            f32(bulk_rows, LANES),
            f32(late_rows, LANES),
            f32(peers - 1, bulk_rows // peers, LANES),
            f32(peers - 1, late_rows, LANES),
            f32(bulk_rows // peers, LANES),
            f32(bulk_rows, LANES),
            f32(chunks, rows, LANES),
            f32(groups, cap, rows),
            dma(chunks + 4),
            dma(3),
            dma(1),
            dma((chunks - 1) * (full + 1) + len(edges) - 1),
            dma(4),
            dma(3, 2),
            pltpu.SemaphoreType.REGULAR((max(2, groups.bit_length()),)),
        ],
        compiler_params=pltpu.CompilerParams(
            collective_id=0, has_side_effects=True, vmem_limit_bytes=LIMIT
        ),
    )(
        profiles.T,
        courant.T,
        owner_map.reshape(groups * chunks, LANES),
        cloud_flags[None, :],
        crm_state,
    )
    tendency, final = pl.pallas_call(
        finish_kernel,
        out_shape=(
            jax.ShapeDtypeStruct((fields * levels, columns), jnp.float32),
            jax.ShapeDtypeStruct(crm_state.shape, jnp.float32),
        ),
        in_specs=[anywhere] * 3,
        out_specs=(anywhere,) * 2,
        scratch_shapes=[
            f32(groups, cap, rows),
            f32(groups * cap, columns),
            f32(*crm_state.shape),
            f32(fields * levels, columns),
            dma(2 + PIECES * fields),
            dma(1 + PIECES * fields),
        ],
        compiler_params=pltpu.CompilerParams(vmem_limit_bytes=LIMIT),
    )(land, give, state)
    return tendency.T, final


def solution(mesh):
    placed = (P("col", None), P("col", None), P(), P("col"), P(None, None, "grp", "col"))
    return jax.shard_map(
        on_device,
        mesh=mesh,
        in_specs=placed,
        out_specs=(P("col", None), P(None, None, "grp", "col")),
        check_vma=False,
    )
```
